32 devices in a mesh: ang: 16 (over z, y, core), sl: 2 (over x).
Axes of the slice: x: 2, y: 2, z: 4, core: 2. Of those that a mesh axis runs over, the one named last changes fastest.
Arguments:
- sinogram: bfloat16 [16, 32, 1024], P('sl', 'ang'), may hold values from -72 to 72
- detector_coord: int32 [32, 32, 512], P('ang', 'sl'), may hold values from 0 to 1072693247
Outputs:
- image_rows: float32 [32, 16, 512], P('ang', 'sl')
The draws below stay inside these ranges and needn't reach their ends.
All inputs are finite; a program needn't handle non-finite values.
Results may differ from the reference program's by a relative error of at most 0.0052.
Values may be sent and summed in bfloat16 or wider, within the bound.
A program may use at most 64 MiB of HBM per device.

```python
import math
import jax
import jax.numpy as jnp
from jax import lax

BINS = 1024
IMG = 512
SLICES = 16
ANGLES = 32
ROWS = 32


def place_ends(result, own_key, least, high):
    index_at = [jax.random.randint(jax.random.fold_in(own_key, axis), (), 0, length) for axis, length in enumerate(result.shape)]
    longest = result.shape.index(max(result.shape))
    beside = index_at[:longest] + [(index_at[longest] + 1) % result.shape[longest]] + index_at[longest + 1:]
    return result.at[tuple(index_at)].set(least).at[tuple(beside)].set(high)


def levels(key, shape, split, low, high):
    gain, own = 1.0, jax.random.fold_in(key, 6)
    for dim, parts in split:
        heights = jnp.exp(jax.random.uniform(jax.random.fold_in(own, dim), (parts,), jnp.float32, low / len(split), high / len(split)))
        gain = gain * jnp.repeat(heights, shape[dim] // parts).reshape([-1 if axis == dim else 1 for axis in range(len(shape))])
    return gain


def bell_draw(rng, dims, scale, reach, shards=(), kind=jnp.bfloat16):
    values = scale * jax.random.normal(rng, dims, jnp.float32)
    if shards:
        values = values * levels(rng, dims, shards, -0.22, 0.18)
    return jnp.clip(values, -reach, reach).astype(kind)


def setup_inputs(seed: int = 0) -> dict:
    key_list = jax.random.split(jax.random.key(seed), 3)
    return {
        "sinogram": bell_draw(key_list[0], (SLICES, ANGLES, BINS), 12.0, 72.0, ((0, 2), (1, 16))),
        "detector_coord": place_ends(jax.random.randint(key_list[1], (ANGLES, ROWS, IMG), 0, (BINS - 1) * 1048576), jax.random.fold_in(key_list[1], 1), 0, ((BINS - 1) * 1048576) - 1).astype(jnp.int32),
    }


def ramp_table(bin_count):
    first = lax.broadcasted_iota(jnp.int32, (bin_count, bin_count), 0)
    second = lax.broadcasted_iota(jnp.int32, (bin_count, bin_count), 1)
    offset = second - first
    offset_sq = jnp.maximum((offset * offset).astype(jnp.float32), jnp.float32(1.0))
    odd_mask = (offset % 2) != 0
    values = jnp.where(offset == 0, jnp.float32(0.25), jnp.where(odd_mask, jnp.float32(-1.0 / (math.pi ** 2)) / offset_sq, jnp.float32(0.0)))
    return values.astype(jnp.bfloat16)


def interp_weights(row_coords, bin_count):
    bin_left = row_coords // 1048576
    fraction = (row_coords % 1048576).astype(jnp.float32) / jnp.float32(1048576.0)
    positions = lax.broadcasted_iota(jnp.int32, row_coords.shape + (bin_count,), 2)
    left_part = jnp.where(positions == bin_left[..., None], 1.0 - fraction[..., None], jnp.float32(0.0))
    right_part = jnp.where(positions == bin_left[..., None] + 1, fraction[..., None], jnp.float32(0.0))
    return (left_part + right_part).astype(jnp.bfloat16)


def reference(sinogram, detector_coord):
    slices, angles, bin_count = sinogram.shape
    table = ramp_table(bin_count)
    filtered = jnp.dot(sinogram.reshape(slices * angles, bin_count), table, preferred_element_type=jnp.float32)
    filtered = filtered.astype(jnp.bfloat16).reshape(slices, angles, bin_count)

    def add_angle(running, angle_step):
        projection = lax.dynamic_index_in_dim(filtered, angle_step, 1, keepdims=False)
        row_coords = lax.dynamic_index_in_dim(detector_coord, angle_step, 0, keepdims=False)
        weights = interp_weights(row_coords, bin_count)
        contrib = jnp.einsum('rxb,sb->rsx', weights.astype(jnp.float32), projection.astype(jnp.float32))
        return running + contrib, None

    start_value = jnp.zeros((detector_coord.shape[1], slices, detector_coord.shape[2]), jnp.float32)
    running, unused = lax.scan(add_angle, start_value, jnp.arange(angles, dtype=jnp.int32))
    return running * jnp.float32(math.pi / angles)
```

```python
import functools
import math

import jax
import jax.numpy as jnp
from jax import lax
from jax.experimental import pallas as pl
from jax.experimental.pallas import tpu as pltpu
from jax.sharding import PartitionSpec as P

LANES = 128
SUBLANES = 8
CORES = 2
FRACTION_BITS = 20
MESH = pl.DeviceIdType.MESH
ALONG_LANES = lax.GatherDimensionNumbers(
    offset_dims=(),
    collapsed_slice_dims=(1,),
    start_index_map=(1,),
    operand_batching_dims=(0,),
    start_indices_batching_dims=(0,),
)


def build_strip(strip, bins):
    row = lax.broadcasted_iota(jnp.int32, strip.shape, 0)
    lane = lax.broadcasted_iota(jnp.int32, strip.shape, 1)
    offset = lane - row + (bins - LANES)
    wide = offset.astype(jnp.float32)
    square = jnp.maximum(wide * wide, jnp.float32(1.0))
    odd = jnp.where((offset & 1) != 0, jnp.float32(-1.0 / math.pi**2) / square, jnp.float32(0.0))
    strip[...] = jnp.where(offset == 0, jnp.float32(0.25), odd).astype(jnp.bfloat16)


def filter_rows(sino, strip, rows_f, size):
    slices, angles, bins = sino.shape
    rows, count = slices * angles, bins // size
    blocks = [sino[:, :, i * size : (i + 1) * size].reshape(rows, size) for i in range(count)]
    totals = [None] * count
    for d in range(1 - count, count):
        inner = [i for i in range(count) if 0 <= i + d < count]
        first = bins - LANES - size * d
        right = jnp.concatenate(
            [strip[first - u : first - u + size, :] for u in range(0, size, LANES)], axis=1
        )
        left = jnp.concatenate([blocks[i] for i in inner], axis=0)
        part = jnp.dot(left, right, preferred_element_type=jnp.float32)
        for at, i in enumerate(inner):
            piece = part[at * rows : (at + 1) * rows]
            totals[i + d] = piece if totals[i + d] is None else totals[i + d] + piece
    for j, total in enumerate(totals):
        total = total.astype(jnp.bfloat16).astype(jnp.float32)
        for u in range(0, size, LANES):
            at = (j * size + u) // LANES * rows
            rows_f[at : at + rows, :] = total[:, u : u + LANES]


def build_tables(rows_f, tables_f, slices, angles):
    levels = rows_f.shape[0] // (slices * angles)
    bins = levels * LANES
    for a in range(angles):
        starts = [level * slices * angles + a for level in range(levels)]
        here = jnp.concatenate(
            [rows_f[pl.ds(at, slices, stride=angles), :] for at in starts], axis=1
        )
        following = pltpu.roll(here, bins - 1, 1)
        for v, value in enumerate((here, following)):
            for level in range(levels):
                at = pl.ds(level * angles + a, slices, stride=levels * angles)
                tables_f[v, at, :] = value[:, level * LANES : (level + 1) * LANES]


def pick(table, index):
    return lax.gather(
        table, index[..., None], ALONG_LANES, (1, 1),
        mode=lax.GatherScatterMode.PROMISE_IN_BOUNDS,
    )


def spot_weights(lines, group):
    angles = len(lines)
    row = lax.broadcasted_iota(jnp.int32, (SUBLANES, LANES), 0)
    value = jnp.broadcast_to(lines[0], (SUBLANES, LANES))
    for a in range(1, angles):
        value = jnp.where(row % angles == a, jnp.broadcast_to(lines[a], (SUBLANES, LANES)), value)
    left = value >> FRACTION_BITS
    lane, level = left & (LANES - 1), left >> 7
    right_w = (value & (2**FRACTION_BITS - 1)).astype(jnp.float32) * jnp.float32(2.0**-FRACTION_BITS)
    left_w = 1.0 - right_w
    masks = [level == (row + at) // angles for at in range(0, group, SUBLANES)]

    def stack(parts):
        return jnp.concatenate(parts, axis=0)

    return (
        stack([lane] * len(masks)).astype(jnp.int16),
        stack([jnp.where(m, left_w, 0.0) for m in masks]).astype(jnp.bfloat16),
        stack([jnp.where(m, right_w, 0.0) for m in masks]).astype(jnp.bfloat16),
    )


def fold(value):
    value = value.astype(jnp.float32)
    total = value[:SUBLANES]
    for at in range(SUBLANES, value.shape[0], SUBLANES):
        total = total + value[at : at + SUBLANES]
    return total


def spot_sums(tables, lines, slices, sums):
    group = tables.shape[1] // slices
    index, left_w, right_w = spot_weights(lines, group)
    result = []
    for s in range(slices):
        at = slice(s * group, (s + 1) * group)
        value = fold(left_w * pick(tables[0, at, :], index) + right_w * pick(tables[1, at, :], index))
        result.append(value if sums is None else sums[s] + value)
    return result


def add_rows(sums):
    row = lax.broadcasted_iota(jnp.int32, (SUBLANES, LANES), 0)

    def join(a, b, shift):
        low = (row & shift) == 0
        return jnp.where(low, a + pltpu.roll(a, SUBLANES - shift, 0), b + pltpu.roll(b, shift, 0))

    done = []
    for start in range(0, len(sums), SUBLANES):
        part = sums[start : start + SUBLANES]
        part = part + [jnp.zeros_like(part[0])] * (SUBLANES - len(part))
        for shift in (4, 2, 1):
            part = [join(part[i], part[i + shift], shift) for i in range(shift)]
        done.append(part[0])
    done = done[0] if len(done) == 1 else jnp.concatenate(done, axis=0)
    return done[: len(sums)]


def kernel(
    groups, halves, row_share, sino_hbm, coord_hbm, out, sino, strip, rows_f, tables_f, tables,
    coords, stage, early, send, recv, local_sem, t_send, t_recv, c_send, c_recv, p_send, p_recv,
):
    me, half = lax.axis_index("ang"), lax.axis_index("sl")
    core = lax.rem(me, CORES)
    mate = me + 1 - 2 * core
    slices, angles, bins = sino.shape
    tiles, per_tile, columns = coords.shape[3:]
    share = tiles * per_tile // row_share
    across = columns // LANES

    own_side = coord_hbm.at[:, :, :, pl.ds(pl.multiple_of(core * columns, LANES), columns)]
    mate_side = coord_hbm.at[:, :, :, pl.ds(pl.multiple_of((1 - core) * columns, LANES), columns)]
    get_sino = pltpu.make_async_copy(sino_hbm, sino, local_sem.at[0])
    get_own = pltpu.make_async_copy(own_side, coords.at[half, core], local_sem.at[1])
    get_mate = pltpu.make_async_copy(mate_side, stage, local_sem.at[2])
    get_sino.start()
    get_own.start()
    get_mate.start()

    barrier = pltpu.get_barrier_semaphore()

    def signal(ang, sl):
        pl.semaphore_signal(barrier, inc=1, device_id={"ang": ang, "sl": sl}, device_id_type=MESH)

    for k in range(1, groups):
        signal(lax.rem(me + k, groups), half)
    for t in range(1, halves):
        signal(me, lax.rem(half + t, halves))
        signal(mate, lax.rem(half + t, halves))

    build_strip(strip, bins)
    get_sino.wait()
    filter_rows(sino, strip, rows_f, 2 * LANES)
    build_tables(rows_f, tables_f, slices, angles)
    for v in range(2):
        tables[core, v] = tables_f[v].astype(jnp.bfloat16)
    get_own.wait()
    get_mate.wait()
    pl.semaphore_wait(barrier, groups - 1 + CORES * (halves - 1))

    def remote(source, target, send_sem, recv_sem, ang, sl):
        return pltpu.make_async_remote_copy(
            src_ref=source, dst_ref=target, send_sem=send_sem, recv_sem=recv_sem,
            device_id={"ang": ang, "sl": sl}, device_id_type=MESH,
        )

    inputs = [
        remote(tables.at[core], tables.at[core], t_send, t_recv, mate, half),
        remote(stage, coords.at[half, core], c_send.at[0], c_recv.at[half, core], mate, half),
    ]
    for t in range(1, halves):
        side = lax.rem(half + t, halves)
        inputs.append(remote(
            coords.at[half, core], coords.at[half, core], c_send.at[2 * t - 1],
            c_recv.at[half, core], me, side,
        ))
        inputs.append(remote(
            stage, coords.at[half, core], c_send.at[2 * t], c_recv.at[half, core], mate, side,
        ))
    for copy in inputs:
        copy.start()

    def lines(t, k, tile, r, x):
        return [
            coords[t, k, a, tile, r : r + 1, x * LANES : (x + 1) * LANES] for a in range(angles)
        ]

    spots = [(r, x) for r in range(per_tile) for x in range(across)]

    def own_angles(tile, carry):
        for r, x in spots:
            sums = spot_sums(tables.at[core], lines(half, core, tile, r, x), slices, None)
            for s in range(slices):
                early[tile, r * across + x, s] = sums[s]
        return carry

    lax.fori_loop(0, tiles, own_angles, 0)

    def part_copy(owner):
        return remote(
            send.at[owner], recv.at[me], p_send.at[owner], p_recv.at[me], owner, half
        )

    def deliver(t, tile, done):
        for o in range(per_tile // row_share):
            owner = t * share + tile * (per_tile // row_share) + o
            value = jnp.concatenate(
                [
                    jnp.concatenate([done[o * row_share + i, x] for x in range(across)], axis=1)
                    for i in range(row_share)
                ],
                axis=0,
            ).astype(jnp.bfloat16)

            @pl.when(owner == me)
            def _():
                recv[me] = value

            @pl.when(owner != me)
            def _():
                send[owner] = value
                part_copy(owner).start()

    inputs[0].wait_recv()

    def coords_arrived(t, k):
        pltpu.make_async_copy(stage, coords.at[t, k], c_recv.at[t, k]).wait()

    coords_arrived(half, 1 - core)

    def mate_angles(tile, carry):
        done = {}
        for r, x in spots:
            sums = [early[tile, r * across + x, s] for s in range(slices)]
            done[r, x] = add_rows(spot_sums(
                tables.at[1 - core], lines(half, 1 - core, tile, r, x), slices, sums
            ))
        deliver(half, tile, done)
        return carry

    lax.fori_loop(0, tiles, mate_angles, 0)

    for t in range(1, halves):
        side = lax.rem(half + t, halves)
        for k in range(CORES):
            coords_arrived(side, k)

        def all_angles(tile, carry):
            done = {}
            for r, x in spots:
                sums = None
                for k in range(CORES):
                    sums = spot_sums(tables.at[k], lines(side, k, tile, r, x), slices, sums)
                done[r, x] = add_rows(sums)
            deliver(side, tile, done)
            return carry

        lax.fori_loop(0, tiles, all_angles, 0)

    for k in range(1, groups):
        source = lax.rem(me + k, groups)
        remote(send.at[0], recv.at[source], p_send.at[0], p_recv.at[source], mate, half).wait_recv()
    scale = jnp.float32(math.pi / (angles * groups))
    for c in range(CORES):
        total = None
        for chip in range(groups // CORES):
            value = recv[chip * CORES + c].astype(jnp.float32)
            total = value if total is None else total + value
        total = total * scale
        for i in range(row_share):
            out[i, :, c * columns : (c + 1) * columns] = total[i * slices : (i + 1) * slices]
    for copy in inputs:
        copy.wait_send()
    for k in range(1, groups):
        part_copy(lax.rem(me + k, groups)).wait_send()


def shards(sinogram, detector_coord):
    slices, angles, bins = sinogram.shape
    local_rows, width = detector_coord.shape[1:]
    groups, halves = lax.axis_size("ang"), lax.axis_size("sl")
    row_share = local_rows * halves // groups
    tiles, columns = local_rows // SUBLANES, width // CORES
    group = bins // LANES * angles
    coords = detector_coord.reshape(angles, tiles, SUBLANES, width)
    block = (angles, tiles, SUBLANES, columns)
    message = (groups, row_share * slices, columns)
    spots = SUBLANES * columns // LANES
    dma = pltpu.SemaphoreType.DMA
    return pl.pallas_call(
        functools.partial(kernel, groups, halves, row_share),
        out_shape=pltpu.VMEM((row_share, slices, width), jnp.float32),
        in_specs=[pl.BlockSpec(memory_space=pl.ANY)] * 2,
        out_specs=pl.BlockSpec(memory_space=pltpu.VMEM),
        scratch_shapes=[
            pltpu.VMEM(sinogram.shape, sinogram.dtype),
            pltpu.VMEM((2 * bins - LANES, LANES), jnp.bfloat16),
            pltpu.VMEM((slices * group, LANES), jnp.float32),
            pltpu.VMEM((2, slices * group, LANES), jnp.float32),
            pltpu.VMEM((CORES, 2, slices * group, LANES), jnp.bfloat16),
            pltpu.VMEM((halves, CORES) + block, jnp.int32),
            pltpu.VMEM(block, jnp.int32),
            pltpu.VMEM((tiles, spots, slices, SUBLANES, LANES), jnp.float32),
            pltpu.VMEM(message, jnp.bfloat16),
            pltpu.VMEM(message, jnp.bfloat16),
            dma((3,)),
            dma(()),
            dma(()),
            dma((2 * halves - 1,)),
            dma((halves, CORES)),
            dma((groups,)),
            dma((groups,)),
        ],
        compiler_params=pltpu.CompilerParams(collective_id=0, has_side_effects=True),
    )(sinogram, coords)


def solution(mesh):
    in_specs = (P("sl", "ang", None), P("ang", "sl", None))
    out_specs = P("ang", "sl", None)
    return jax.shard_map(shards, mesh=mesh, in_specs=in_specs, out_specs=out_specs, check_vma=False)
```

```python
import functools
import math

import jax
import jax.numpy as jnp
from jax import lax
from jax.experimental import pallas as pl
from jax.experimental.pallas import tpu as pltpu
from jax.sharding import PartitionSpec as P

LANES = 128
SUBLANES = 8
CORES = 2
FRACTION_BITS = 20
MESH = pl.DeviceIdType.MESH
ALONG_LANES = lax.GatherDimensionNumbers(
    offset_dims=(),
    collapsed_slice_dims=(1,),
    start_index_map=(1,),
    operand_batching_dims=(0,),
    start_indices_batching_dims=(0,),
)


def build_strip(strip, bins):
    row = lax.broadcasted_iota(jnp.int32, strip.shape, 0)
    lane = lax.broadcasted_iota(jnp.int32, strip.shape, 1)
    offset = lane - row + (bins - LANES)
    wide = offset.astype(jnp.float32)
    square = jnp.maximum(wide * wide, jnp.float32(1.0))
    odd = jnp.where((offset & 1) != 0, jnp.float32(-1.0 / math.pi**2) / square, jnp.float32(0.0))
    strip[...] = jnp.where(offset == 0, jnp.float32(0.25), odd).astype(jnp.bfloat16)


def filter_rows(sino, strip, rows_f, size):
    slices, angles, bins = sino.shape
    rows, count = slices * angles, bins // size
    blocks = [sino[:, :, i * size : (i + 1) * size].reshape(rows, size) for i in range(count)]
    totals = [None] * count
    for d in range(1 - count, count):
        inner = [i for i in range(count) if 0 <= i + d < count]
        first = bins - LANES - size * d
        right = jnp.concatenate(
            [strip[first - u : first - u + size, :] for u in range(0, size, LANES)], axis=1
        )
        left = jnp.concatenate([blocks[i] for i in inner], axis=0)
        part = jnp.dot(left, right, preferred_element_type=jnp.float32)
        for at, i in enumerate(inner):
            piece = part[at * rows : (at + 1) * rows]
            totals[i + d] = piece if totals[i + d] is None else totals[i + d] + piece
    for j, total in enumerate(totals):
        total = total.astype(jnp.bfloat16).astype(jnp.float32)
        for u in range(0, size, LANES):
            at = (j * size + u) // LANES * rows
            rows_f[at : at + rows, :] = total[:, u : u + LANES]


def build_tables(rows_f, tables_f, slices, angles):
    levels = rows_f.shape[0] // (slices * angles)
    bins = levels * LANES
    for a in range(angles):
        starts = [level * slices * angles + a for level in range(levels)]
        here = jnp.concatenate(
            [rows_f[pl.ds(at, slices, stride=angles), :] for at in starts], axis=1
        )
        following = pltpu.roll(here, bins - 1, 1)
        for v, value in enumerate((here, following)):
            for level in range(levels):
                at = pl.ds(level * angles + a, slices, stride=levels * angles)
                tables_f[v, at, :] = value[:, level * LANES : (level + 1) * LANES]


def pick(table, index):
    return lax.gather(
        table, index[..., None], ALONG_LANES, (1, 1),
        mode=lax.GatherScatterMode.PROMISE_IN_BOUNDS,
    )


def spot_weights(lines, group):
    angles = len(lines)
    row = lax.broadcasted_iota(jnp.int32, (SUBLANES, LANES), 0)
    value = jnp.broadcast_to(lines[0], (SUBLANES, LANES))
    for a in range(1, angles):
        value = jnp.where(row % angles == a, jnp.broadcast_to(lines[a], (SUBLANES, LANES)), value)
    left = value >> FRACTION_BITS
    lane, level = left & (LANES - 1), left >> 7
    right_w = (value & (2**FRACTION_BITS - 1)).astype(jnp.float32) * jnp.float32(2.0**-FRACTION_BITS)
    left_w = 1.0 - right_w
    masks = [level == (row + at) // angles for at in range(0, group, SUBLANES)]

    def stack(parts):
        return jnp.concatenate(parts, axis=0)

    return (
        stack([lane] * len(masks)).astype(jnp.int16),
        stack([jnp.where(m, left_w, 0.0) for m in masks]).astype(jnp.bfloat16),
        stack([jnp.where(m, right_w, 0.0) for m in masks]).astype(jnp.bfloat16),
    )


def fold(value):
    value = value.astype(jnp.float32)
    total = value[:SUBLANES]
    for at in range(SUBLANES, value.shape[0], SUBLANES):
        total = total + value[at : at + SUBLANES]
    return total


def spot_sums(tables, lines, slices, sums):
    group = tables.shape[1] // slices
    index, left_w, right_w = spot_weights(lines, group)
    result = []
    for s in range(slices):
        at = slice(s * group, (s + 1) * group)
        value = fold(left_w * pick(tables[0, at, :], index) + right_w * pick(tables[1, at, :], index))
        result.append(value if sums is None else sums[s] + value)
    return result


def add_rows(sums):
    row = lax.broadcasted_iota(jnp.int32, (SUBLANES, LANES), 0)

    def join(a, b, shift):
        low = (row & shift) == 0
        return jnp.where(low, a + pltpu.roll(a, SUBLANES - shift, 0), b + pltpu.roll(b, shift, 0))

    done = []
    for start in range(0, len(sums), SUBLANES):
        part = sums[start : start + SUBLANES]
        part = part + [jnp.zeros_like(part[0])] * (SUBLANES - len(part))
        for shift in (4, 2, 1):
            part = [join(part[i], part[i + shift], shift) for i in range(shift)]
        done.append(part[0])
    done = done[0] if len(done) == 1 else jnp.concatenate(done, axis=0)
    return done[: len(sums)]


def kernel(
    groups, halves, row_share, sino_hbm, coord_hbm, out, sino, strip, rows_f, tables_f, tables,
    coords, stage, early, send, recv, local_sem, t_send, t_recv, c_send, c_recv, p_send, p_recv, lower_sem, upper_sem,
):
    me, half = lax.axis_index("ang"), lax.axis_index("sl")
    core = lax.rem(me, CORES)
    mate = me + 1 - 2 * core
    slices, angles, bins = sino.shape
    tiles, _, per_tile, columns = coords.shape[2:]
    share = tiles * per_tile // row_share
    across = columns // LANES

    def local_coords(tile, side, target, sem):
        at = pl.ds(pl.multiple_of(side * columns, LANES), columns)
        return pltpu.make_async_copy(coord_hbm.at[:, tile, :, at], target.at[tile], local_sem.at[sem])

    get_sino = pltpu.make_async_copy(sino_hbm, sino, local_sem.at[0])
    get_coords = []
    for tile in range(tiles):
        get_coords.append(local_coords(tile, core, coords.at[half, core], 2 * tile + 1))
        get_coords.append(local_coords(tile, 1 - core, stage, 2 * tile + 2))
    get_sino.start()
    for copy in get_coords:
        copy.start()

    quad = 2 * CORES
    place, places = me // quad, groups // quad
    barrier = pltpu.get_barrier_semaphore()

    def signal(sem, ang, sl):
        pl.semaphore_signal(sem, inc=1, device_id={"ang": ang, "sl": sl}, device_id_type=MESH)

    for t in range(1, halves):
        signal(barrier, me, lax.rem(half + t, halves))
        signal(barrier, mate, lax.rem(half + t, halves))
    for k in range(1, quad):
        signal(barrier, place * quad + lax.rem(me + k, quad), half)
    has_lower, has_upper = place > 0, place < places - 1

    @pl.when(has_lower)
    def _():
        signal(barrier, me - quad, half)

    @pl.when(has_upper)
    def _():
        signal(barrier, me + quad, half)

    build_strip(strip, bins)
    get_sino.wait()
    filter_rows(sino, strip, rows_f, 2 * LANES)
    build_tables(rows_f, tables_f, slices, angles)
    for v in range(2):
        tables[core, v] = tables_f[v].astype(jnp.bfloat16)
    for copy in get_coords:
        copy.wait()
    beside = has_lower.astype(jnp.int32) + has_upper.astype(jnp.int32)
    pl.semaphore_wait(barrier, quad - 1 + CORES * (halves - 1) + beside)

    @pl.when(jnp.logical_and(place == 0, has_upper))
    def _():
        signal(lower_sem, me + quad, half)

    @pl.when(jnp.logical_and(place == places - 1, has_lower))
    def _():
        signal(upper_sem, me - quad, half)

    def remote(source, target, send_sem, recv_sem, ang, sl):
        return pltpu.make_async_remote_copy(
            src_ref=source, dst_ref=target, send_sem=send_sem, recv_sem=recv_sem,
            device_id={"ang": ang, "sl": sl}, device_id_type=MESH,
        )

    def coord_copy(tile, source, ang, t, which):
        return remote(
            source.at[tile], coords.at[half, core, tile], c_send.at[tile, t, which],
            c_recv.at[half, core, tile], ang, lax.rem(half + t, halves),
        )

    def to_side(tile, t):
        return [
            coord_copy(tile, coords.at[half, core], me, t, 0),
            coord_copy(tile, stage, mate, t, 1),
        ]

    def start_sides(tiles_now):
        for tile in tiles_now:
            for t in range(1, halves):
                for copy in to_side(tile, t):
                    copy.start()

    start_sides(range(1))
    mate_coords = [coord_copy(tile, stage, mate, 0, 1) for tile in range(tiles)]
    for copy in mate_coords:
        copy.start()
    mate_tables = remote(tables.at[core], tables.at[core], t_send, t_recv, mate, half)
    mate_tables.start()

    def lines(t, k, tile, r, x):
        return [
            coords[t, k, tile, a, r : r + 1, x * LANES : (x + 1) * LANES] for a in range(angles)
        ]

    spots = [(r, x) for r in range(per_tile) for x in range(across)]

    middle = jnp.logical_and(has_lower, has_upper)

    def own_angles(tile, carry):
        for r, x in spots:
            sums = spot_sums(tables.at[core], lines(half, core, tile, r, x), slices, None)
            for s in range(slices):
                early[tile, r * across + x, s] = sums[s]

        @pl.when(jnp.logical_and(tile == jnp.clip(place - 1, 0, tiles - 1), middle))
        def _():
            pl.semaphore_wait(lower_sem, 1)
            signal(lower_sem, me + quad, half)

        return carry

    lax.fori_loop(0, tiles, own_angles, 0)
    start_sides(range(1, tiles))

    def part_copy(owner):
        return remote(send.at[owner], recv.at[me], p_send.at[owner], p_recv.at[me], owner, half)

    per_step = per_tile // row_share
    steps = halves * tiles
    beyond = places - 1 - place
    flush = jnp.where(beyond < 3, jnp.minimum(beyond, tiles) - 1, steps - 1)

    def step_owner(step, o):
        t, tile = step // tiles, lax.rem(step, tiles)
        return lax.rem(half + t, halves) * share + tile * per_step + o

    def keep(step, done):
        for o in range(per_step):
            owner = step_owner(step, o)
            value = jnp.concatenate(
                [
                    jnp.concatenate([done[o * row_share + i, x] for x in range(across)], axis=1)
                    for i in range(row_share)
                ],
                axis=0,
            ).astype(jnp.bfloat16)
            send[owner] = value

    def deliver(step, upper):
        for o in range(per_step):
            owner = step_owner(step, o)

            @pl.when(jnp.logical_and(owner != me, (owner // quad > place) == upper))
            def _():
                part_copy(owner).start()

    def hear(step):
        @pl.when(jnp.logical_and(flush == step, has_upper))
        def _():
            pl.semaphore_wait(upper_sem, 1)

            @pl.when(has_lower)
            def _():
                signal(upper_sem, me - quad, half)

        def late(earlier, carry):
            deliver(earlier, True)
            return carry

        lax.fori_loop(jnp.where(flush == step, 0, step), step, late, 0)

    def after(step):
        deliver(step, False)
        hear(step)

        @pl.when(flush <= step)
        def _():
            deliver(step, True)

    hear(-1)
    mate_tables.wait_recv()

    def coords_arrived(t, k, tile):
        pltpu.make_async_copy(stage.at[tile], coords.at[t, k, tile], c_recv.at[t, k, tile]).wait()

    def mate_angles(tile, carry):
        coords_arrived(half, 1 - core, tile)
        done = {}
        for r, x in spots:
            sums = [early[tile, r * across + x, s] for s in range(slices)]
            done[r, x] = add_rows(spot_sums(
                tables.at[1 - core], lines(half, 1 - core, tile, r, x), slices, sums
            ))
        keep(tile, done)

        @pl.when(tile == 0)
        def _():
            @pl.when(jnp.logical_and(has_lower, jnp.logical_not(has_upper)))
            def _():
                pl.semaphore_wait(lower_sem, 1)

        after(tile)
        return carry

    lax.fori_loop(0, tiles, mate_angles, 0)

    def all_angles(step, carry):
        side, tile = lax.rem(half + step // tiles, halves), lax.rem(step, tiles)
        for k in range(CORES):
            coords_arrived(side, k, tile)
        done = {}
        for r, x in spots:
            sums = None
            for k in range(CORES):
                sums = spot_sums(tables.at[k], lines(side, k, tile, r, x), slices, sums)
            done[r, x] = add_rows(sums)
        keep(step, done)
        after(step)
        return carry

    lax.fori_loop(tiles, steps, all_angles, 0)

    for k in range(1, groups):
        source = lax.rem(me + k, groups)
        remote(send.at[0], recv.at[source], p_send.at[0], p_recv.at[source], mate, half).wait_recv()
    recv[me] = send[me]
    scale = jnp.float32(math.pi / (angles * groups))
    for c in range(CORES):
        total = None
        for chip in range(groups // CORES):
            value = recv[chip * CORES + c].astype(jnp.float32)
            total = value if total is None else total + value
        total = total * scale
        for i in range(row_share):
            out[i, :, c * columns : (c + 1) * columns] = total[i * slices : (i + 1) * slices]
    mate_tables.wait_send()
    for copy in mate_coords:
        copy.wait_send()
    for tile in range(tiles):
        for t in range(1, halves):
            for copy in to_side(tile, t):
                copy.wait_send()
    for k in range(1, groups):
        part_copy(lax.rem(me + k, groups)).wait_send()


def shards(sinogram, detector_coord):
    slices, angles, bins = sinogram.shape
    local_rows, width = detector_coord.shape[1:]
    groups, halves = lax.axis_size("ang"), lax.axis_size("sl")
    row_share = local_rows * halves // groups
    tiles, columns = local_rows // SUBLANES, width // CORES
    group = bins // LANES * angles
    coords = detector_coord.reshape(angles, tiles, SUBLANES, width)
    block = (tiles, angles, SUBLANES, columns)
    message = (groups, row_share * slices, columns)
    spots = SUBLANES * columns // LANES
    dma = pltpu.SemaphoreType.DMA
    return pl.pallas_call(
        functools.partial(kernel, groups, halves, row_share),
        out_shape=pltpu.VMEM((row_share, slices, width), jnp.float32),
        in_specs=[pl.BlockSpec(memory_space=pl.ANY)] * 2,
        out_specs=pl.BlockSpec(memory_space=pltpu.VMEM),
        scratch_shapes=[
            pltpu.VMEM(sinogram.shape, sinogram.dtype),
            pltpu.VMEM((2 * bins - LANES, LANES), jnp.bfloat16),
            pltpu.VMEM((slices * group, LANES), jnp.float32),
            pltpu.VMEM((2, slices * group, LANES), jnp.float32),
            pltpu.VMEM((CORES, 2, slices * group, LANES), jnp.bfloat16),
            pltpu.VMEM((halves, CORES) + block, jnp.int32),
            pltpu.VMEM(block, jnp.int32),
            pltpu.VMEM((tiles, spots, slices, SUBLANES, LANES), jnp.float32),
            pltpu.VMEM(message, jnp.bfloat16),
            pltpu.VMEM(message, jnp.bfloat16),
            dma((2 * tiles + 1,)),
            dma(()),
            dma(()),
            dma((tiles, halves, 2)),
            dma((halves, CORES, tiles)),
            dma((groups,)),
            dma((groups,)),
            pltpu.SemaphoreType.REGULAR,
            pltpu.SemaphoreType.REGULAR,
        ],
        compiler_params=pltpu.CompilerParams(collective_id=0, has_side_effects=True),
    )(sinogram, coords)


def solution(mesh):
    in_specs = (P("sl", "ang", None), P("ang", "sl", None))
    out_specs = P("ang", "sl", None)
    return jax.shard_map(shards, mesh=mesh, in_specs=in_specs, out_specs=out_specs, check_vma=False)
```

```python
import functools
import math

import jax
import jax.numpy as jnp
from jax import lax
from jax.experimental import pallas as pl
from jax.experimental.pallas import tpu as pltpu
from jax.sharding import PartitionSpec as P

LANES = 128
SUBLANES = 8
CORES = 2
PARTS = 2
FRACTION_BITS = 20
MESH = pl.DeviceIdType.MESH
ALONG_LANES = lax.GatherDimensionNumbers(
    offset_dims=(),
    collapsed_slice_dims=(1,),
    start_index_map=(1,),
    operand_batching_dims=(0,),
    start_indices_batching_dims=(0,),
)


def build_strip(strip, bins):
    row = lax.broadcasted_iota(jnp.int32, strip.shape, 0)
    lane = lax.broadcasted_iota(jnp.int32, strip.shape, 1)
    offset = lane - row + (bins - LANES)
    wide = offset.astype(jnp.float32)
    square = jnp.maximum(wide * wide, jnp.float32(1.0))
    odd = jnp.where((offset & 1) != 0, jnp.float32(-1.0 / math.pi**2) / square, jnp.float32(0.0))
    strip[...] = jnp.where(offset == 0, jnp.float32(0.25), odd).astype(jnp.bfloat16)


def filter_rows(sino, strip, rows_f, size):
    slices, angles, bins = sino.shape
    rows, count = slices * angles, bins // size
    blocks = [sino[:, :, i * size : (i + 1) * size].reshape(rows, size) for i in range(count)]
    totals = [None] * count
    for d in range(1 - count, count):
        inner = [i for i in range(count) if 0 <= i + d < count]
        first = bins - LANES - size * d
        right = jnp.concatenate(
            [strip[first - u : first - u + size, :] for u in range(0, size, LANES)], axis=1
        )
        left = jnp.concatenate([blocks[i] for i in inner], axis=0)
        part = jnp.dot(left, right, preferred_element_type=jnp.float32)
        for at, i in enumerate(inner):
            piece = part[at * rows : (at + 1) * rows]
            totals[i + d] = piece if totals[i + d] is None else totals[i + d] + piece
    for j, total in enumerate(totals):
        total = total.astype(jnp.bfloat16).astype(jnp.float32)
        for u in range(0, size, LANES):
            at = (j * size + u) // LANES * rows
            rows_f[at : at + rows, :] = total[:, u : u + LANES]


def build_tables(rows_f, tables_f, slices, angles):
    levels = rows_f.shape[0] // (slices * angles)
    bins = levels * LANES
    for a in range(angles):
        starts = [level * slices * angles + a for level in range(levels)]
        here = jnp.concatenate(
            [rows_f[pl.ds(at, slices, stride=angles), :] for at in starts], axis=1
        )
        following = pltpu.roll(here, bins - 1, 1)
        for v, value in enumerate((here, following)):
            for level in range(levels):
                at = pl.ds(level * angles + a, slices, stride=levels * angles)
                tables_f[v, at, :] = value[:, level * LANES : (level + 1) * LANES]


def pick(table, index):
    return lax.gather(
        table, index[..., None], ALONG_LANES, (1, 1),
        mode=lax.GatherScatterMode.PROMISE_IN_BOUNDS,
    )


def spot_weights(lines, group):
    angles = len(lines)
    row = lax.broadcasted_iota(jnp.int32, (SUBLANES, LANES), 0)
    value = jnp.broadcast_to(lines[0], (SUBLANES, LANES))
    for a in range(1, angles):
        value = jnp.where(row % angles == a, jnp.broadcast_to(lines[a], (SUBLANES, LANES)), value)
    left = value >> FRACTION_BITS
    lane, level = left & (LANES - 1), left >> 7
    right_w = (value & (2**FRACTION_BITS - 1)).astype(jnp.float32) * jnp.float32(2.0**-FRACTION_BITS)
    left_w = 1.0 - right_w
    masks = [level == (row + at) // angles for at in range(0, group, SUBLANES)]

    def stack(parts):
        return jnp.concatenate(parts, axis=0)

    return (
        stack([lane] * len(masks)).astype(jnp.int16),
        stack([jnp.where(m, left_w, 0.0) for m in masks]).astype(jnp.bfloat16),
        stack([jnp.where(m, right_w, 0.0) for m in masks]).astype(jnp.bfloat16),
    )


def fold(value):
    value = value.astype(jnp.float32)
    total = value[:SUBLANES]
    for at in range(SUBLANES, value.shape[0], SUBLANES):
        total = total + value[at : at + SUBLANES]
    return total


def spot_sums(tables, lines, slices, sums):
    group = tables.shape[1] // slices
    index, left_w, right_w = spot_weights(lines, group)
    result = []
    for s in range(slices):
        at = slice(s * group, (s + 1) * group)
        value = fold(left_w * pick(tables[0, at, :], index) + right_w * pick(tables[1, at, :], index))
        result.append(value if sums is None else sums[s] + value)
    return result


def add_rows(sums):
    row = lax.broadcasted_iota(jnp.int32, (SUBLANES, LANES), 0)

    def join(a, b, shift):
        low = (row & shift) == 0
        return jnp.where(low, a + pltpu.roll(a, SUBLANES - shift, 0), b + pltpu.roll(b, shift, 0))

    done = []
    for start in range(0, len(sums), SUBLANES):
        part = sums[start : start + SUBLANES]
        part = part + [jnp.zeros_like(part[0])] * (SUBLANES - len(part))
        for shift in (4, 2, 1):
            part = [join(part[i], part[i + shift], shift) for i in range(shift)]
        done.append(part[0])
    done = done[0] if len(done) == 1 else jnp.concatenate(done, axis=0)
    return done[: len(sums)]


def kernel(
    groups, halves, row_share, sino_hbm, coord_hbm, out, sino, strip, rows_f, tables_f, tables,
    coords, stage, early, send, recv, local_sem, t_send, t_recv, c_send, c_recv, p_send, p_recv, lower_sem, upper_sem,
):
    me, half = lax.axis_index("ang"), lax.axis_index("sl")
    core = lax.rem(me, CORES)
    mate = me + 1 - 2 * core
    slices, angles, bins = sino.shape
    tiles, _, per_tile, columns = stage.shape
    share = tiles * per_tile // row_share
    across = columns // LANES

    def block(t, tile, k):
        return coords.at[(t * tiles + tile) * CORES + k]

    def local_coords(tile, side, target):
        at = pl.ds(pl.multiple_of(side * columns, LANES), columns)
        return pltpu.make_async_copy(coord_hbm.at[:, tile, :, at], target, local_sem.at[1])

    get_sino = pltpu.make_async_copy(sino_hbm, sino, local_sem.at[0])
    get_coords = []
    for tile in range(tiles):
        get_coords.append(local_coords(tile, core, block(half, tile, core)))
        get_coords.append(local_coords(tile, 1 - core, stage.at[tile]))
    get_sino.start()
    for copy in get_coords:
        copy.start()

    quad = 2 * CORES
    place, places = me // quad, groups // quad
    barrier = pltpu.get_barrier_semaphore()

    def signal(sem, ang, sl):
        pl.semaphore_signal(sem, inc=1, device_id={"ang": ang, "sl": sl}, device_id_type=MESH)

    for t in range(1, halves):
        signal(barrier, me, lax.rem(half + t, halves))
        signal(barrier, mate, lax.rem(half + t, halves))
    for k in range(1, quad):
        signal(barrier, place * quad + lax.rem(me + k, quad), half)
    has_lower, has_upper = place > 0, place < places - 1

    @pl.when(has_lower)
    def _():
        signal(barrier, me - quad, half)

    @pl.when(has_upper)
    def _():
        for k in range(quad):
            signal(barrier, (place + 1) * quad + k, half)

    build_strip(strip, bins)
    get_sino.wait()
    filter_rows(sino, strip, rows_f, 2 * LANES)
    build_tables(rows_f, tables_f, slices, angles)
    for v in range(2):
        tables[core, v] = tables_f[v].astype(jnp.bfloat16)
    pair = pl.ds(0, CORES * tiles)
    pltpu.make_async_copy(coords.at[pair], coords.at[pair], local_sem.at[1]).wait()
    beside = quad * has_lower.astype(jnp.int32) + has_upper.astype(jnp.int32)
    pl.semaphore_wait(barrier, quad - 1 + CORES * (halves - 1) + beside)

    @pl.when(jnp.logical_and(place == 1, has_upper))
    def _():
        signal(lower_sem, me + quad, half)

    @pl.when(jnp.logical_and(place == places - 1, has_lower))
    def _():
        signal(upper_sem, me - quad, half)

    def remote(source, target, send_sem, recv_sem, ang, sl):
        return pltpu.make_async_remote_copy(
            src_ref=source, dst_ref=target, send_sem=send_sem, recv_sem=recv_sem,
            device_id={"ang": ang, "sl": sl}, device_id_type=MESH,
        )

    def coord_copy(tile, source, ang, t):
        return remote(
            source, block(half, tile, core), c_send, c_recv.at[half, tile], ang,
            lax.rem(half + t, halves),
        )

    def to_side(tile, t):
        return [
            coord_copy(tile, block(half, tile, core), me, t),
            coord_copy(tile, stage.at[tile], mate, t),
        ]

    def start_sides(tiles_now):
        for tile in tiles_now:
            for t in range(1, halves):
                for copy in to_side(tile, t):
                    copy.start()

    start_sides(range(1))
    mate_coords = [coord_copy(tile, stage.at[tile], mate, 0) for tile in range(tiles)]
    for copy in mate_coords:
        copy.start()
    mate_tables = remote(tables.at[core], tables.at[core], t_send, t_recv, mate, half)
    mate_tables.start()

    def lines(t, k, tile, r, x):
        return [
            coords[
                (t * tiles + tile) * CORES + k, a, r : r + 1, x * LANES : (x + 1) * LANES
            ]
            for a in range(angles)
        ]

    spots = [(r, x) for r in range(per_tile) for x in range(across)]

    def own_angles(tile, carry):
        for r, x in spots:
            sums = spot_sums(tables.at[core], lines(half, core, tile, r, x), slices, None)
            for s in range(slices):
                early[tile, r * across + x, s] = sums[s]

        @pl.when(jnp.logical_and(tile == 0, jnp.logical_and(place > 1, has_upper)))
        def _():
            pl.semaphore_wait(lower_sem, 1)
            signal(lower_sem, me + quad, half)

        return carry

    lax.fori_loop(0, tiles, own_angles, 0)
    start_sides(range(1, tiles))

    def part_copy(owner):
        return remote(send.at[owner], recv.at[me], p_send, p_recv, owner, half)

    per_step = per_tile // row_share
    steps = halves * tiles
    beyond = places - 1 - place
    flush = jnp.where(beyond < 3, jnp.minimum(beyond, tiles) - 1, steps - 1)

    def step_owner(step, o):
        t, tile = step // tiles, lax.rem(step, tiles)
        return lax.rem(half + t, halves) * share + tile * per_step + o

    per_part = max(per_step // PARTS, 1)
    parts = [range(o, o + per_part) for o in range(0, per_step, per_part)]

    def keep(step, owners, done):
        for o in owners:
            value = jnp.concatenate(
                [
                    jnp.concatenate([done[o * row_share + i, x] for x in range(across)], axis=1)
                    for i in range(row_share)
                ],
                axis=0,
            )
            send[step_owner(step, o)] = value.astype(jnp.bfloat16)

    def deliver(step, owners, wanted):
        for o in owners:
            owner = step_owner(step, o)

            @pl.when(jnp.logical_and(owner != me, wanted(owner // quad)))
            def _():
                part_copy(owner).start()

    def hear(step):
        @pl.when(jnp.logical_and(flush == step, has_upper))
        def _():
            pl.semaphore_wait(upper_sem, 1)

            @pl.when(has_lower)
            def _():
                signal(upper_sem, me - quad, half)

        def late(earlier, carry):
            deliver(earlier, range(per_step), lambda to: to > place)
            return carry

        lax.fori_loop(0, jnp.where(flush == step, step + 1, 0), late, 0)

    def hear_lower(step):
        @pl.when(jnp.logical_and(step == 0, jnp.logical_and(place > 1, jnp.logical_not(has_upper))))
        def _():
            pl.semaphore_wait(lower_sem, 1)

    def run_step(step, sums_of, first):
        for owners in parts:
            done = {}
            for o in owners:
                for i in range(row_share):
                    for x in range(across):
                        r = o * row_share + i
                        done[r, x] = add_rows(sums_of(r, x))
            keep(step, owners, done)
            if first and owners is parts[0]:
                hear_lower(step)
            deliver(step, owners, lambda to: jnp.logical_or(to <= place, flush < step))

    hear(-1)
    mate_tables.wait_recv()

    def coords_arrived(t, tile, count):
        at = pl.ds((t * tiles + tile) * CORES, count)
        pltpu.make_async_copy(coords.at[at], coords.at[at], c_recv.at[t, tile]).wait()

    def mate_angles(tile, carry):
        coords_arrived(half, tile, 1)

        def sums_of(r, x):
            sums = [early[tile, r * across + x, s] for s in range(slices)]
            return spot_sums(
                tables.at[1 - core], lines(half, 1 - core, tile, r, x), slices, sums
            )

        run_step(tile, sums_of, True)
        hear(tile)
        return carry

    lax.fori_loop(0, tiles, mate_angles, 0)

    def all_angles(step, carry):
        side, tile = lax.rem(half + step // tiles, halves), lax.rem(step, tiles)
        coords_arrived(side, tile, CORES)

        def sums_of(r, x):
            sums = None
            for k in range(CORES):
                sums = spot_sums(tables.at[k], lines(side, k, tile, r, x), slices, sums)
            return sums

        run_step(step, sums_of, False)
        hear(step)
        return carry

    lax.fori_loop(tiles, steps, all_angles, 0)

    others = pl.ds(0, groups - 1)
    everyone = remote(send.at[others], recv.at[others], p_send, p_recv, mate, half)
    everyone.wait_recv()
    recv[me] = send[me]
    totals = [None] * CORES
    for source in range(groups):
        value = recv[source].astype(jnp.float32)
        c = source % CORES
        totals[c] = value if totals[c] is None else totals[c] + value
    scale = jnp.float32(math.pi / (angles * groups))
    for c in range(CORES):
        total = totals[c] * scale
        for i in range(row_share):
            out[i, :, c * columns : (c + 1) * columns] = total[i * slices : (i + 1) * slices]
    mate_tables.wait_send()
    given = coords.at[pl.ds(0, tiles * (1 + CORES * (halves - 1)))]
    remote(given, given, c_send, c_recv.at[0, 0], mate, half).wait_send()
    everyone.wait_send()


def shards(sinogram, detector_coord):
    slices, angles, bins = sinogram.shape
    local_rows, width = detector_coord.shape[1:]
    groups, halves = lax.axis_size("ang"), lax.axis_size("sl")
    row_share = local_rows * halves // groups
    tiles, columns = local_rows // SUBLANES, width // CORES
    group = bins // LANES * angles
    coords = detector_coord.reshape(angles, tiles, SUBLANES, width)
    block = (angles, SUBLANES, columns)
    message = (groups, row_share * slices, columns)
    spots = SUBLANES * columns // LANES
    dma = pltpu.SemaphoreType.DMA
    return pl.pallas_call(
        functools.partial(kernel, groups, halves, row_share),
        out_shape=pltpu.VMEM((row_share, slices, width), jnp.float32),
        in_specs=[pl.BlockSpec(memory_space=pl.ANY)] * 2,
        out_specs=pl.BlockSpec(memory_space=pltpu.VMEM),
        scratch_shapes=[
            pltpu.VMEM(sinogram.shape, sinogram.dtype),
            pltpu.VMEM((2 * bins - LANES, LANES), jnp.bfloat16),
            pltpu.VMEM((slices * group, LANES), jnp.float32),
            pltpu.VMEM((2, slices * group, LANES), jnp.float32),
            pltpu.VMEM((CORES, 2, slices * group, LANES), jnp.bfloat16),
            pltpu.VMEM((halves * tiles * CORES,) + block, jnp.int32),
            pltpu.VMEM((tiles,) + block, jnp.int32),
            pltpu.VMEM((tiles, spots, slices, SUBLANES, LANES), jnp.float32),
            pltpu.VMEM(message, jnp.bfloat16),
            pltpu.VMEM(message, jnp.bfloat16),
            dma((2,)),
            dma(()),
            dma(()),
            dma(()),
            dma((halves, tiles)),
            dma(()),
            dma(()),
            pltpu.SemaphoreType.REGULAR,
            pltpu.SemaphoreType.REGULAR,
        ],
        compiler_params=pltpu.CompilerParams(collective_id=0, has_side_effects=True),
    )(sinogram, coords)


def solution(mesh):
    in_specs = (P("sl", "ang", None), P("ang", "sl", None))
    out_specs = P("ang", "sl", None)
    return jax.shard_map(shards, mesh=mesh, in_specs=in_specs, out_specs=out_specs, check_vma=False)
```

```python
import functools
import math

import jax
import jax.numpy as jnp
from jax import lax
from jax.experimental import pallas as pl
from jax.experimental.pallas import tpu as pltpu
from jax.sharding import PartitionSpec as P

LANES = 128
SUBLANES = 8
CORES = 2
PARTS = 2
FRACTION_BITS = 20
MESH = pl.DeviceIdType.MESH
ALONG_LANES = lax.GatherDimensionNumbers(
    offset_dims=(),
    collapsed_slice_dims=(1,),
    start_index_map=(1,),
    operand_batching_dims=(0,),
    start_indices_batching_dims=(0,),
)


def build_strip(strip, bins):
    row = lax.broadcasted_iota(jnp.int32, strip.shape, 0)
    lane = lax.broadcasted_iota(jnp.int32, strip.shape, 1)
    offset = lane - row + (bins - LANES)
    wide = offset.astype(jnp.float32)
    square = jnp.maximum(wide * wide, jnp.float32(1.0))
    odd = jnp.where((offset & 1) != 0, jnp.float32(-1.0 / math.pi**2) / square, jnp.float32(0.0))
    strip[...] = jnp.where(offset == 0, jnp.float32(0.25), odd).astype(jnp.bfloat16)


def filter_rows(sino, strip, rows_f, size):
    slices, angles, bins = sino.shape
    rows, count = slices * angles, bins // size
    blocks = [sino[:, :, i * size : (i + 1) * size].reshape(rows, size) for i in range(count)]
    totals = [None] * count
    for d in range(1 - count, count):
        inner = [i for i in range(count) if 0 <= i + d < count]
        first = bins - LANES - size * d
        right = jnp.concatenate(
            [strip[first - u : first - u + size, :] for u in range(0, size, LANES)], axis=1
        )
        left = jnp.concatenate([blocks[i] for i in inner], axis=0)
        part = jnp.dot(left, right, preferred_element_type=jnp.float32)
        for at, i in enumerate(inner):
            piece = part[at * rows : (at + 1) * rows]
            totals[i + d] = piece if totals[i + d] is None else totals[i + d] + piece
    for j, total in enumerate(totals):
        total = total.astype(jnp.bfloat16).astype(jnp.float32)
        for u in range(0, size, LANES):
            at = (j * size + u) // LANES * rows
            rows_f[at : at + rows, :] = total[:, u : u + LANES]


def build_tables(rows_f, tables_f, slices, angles):
    levels = rows_f.shape[0] // (slices * angles)
    bins = levels * LANES
    for a in range(angles):
        starts = [level * slices * angles + a for level in range(levels)]
        here = jnp.concatenate(
            [rows_f[pl.ds(at, slices, stride=angles), :] for at in starts], axis=1
        )
        following = pltpu.roll(here, bins - 1, 1)
        for v, value in enumerate((here, following)):
            for level in range(levels):
                at = pl.ds(level * angles + a, slices, stride=levels * angles)
                tables_f[v, at, :] = value[:, level * LANES : (level + 1) * LANES]


def pick(table, index):
    return lax.gather(
        table, index[..., None], ALONG_LANES, (1, 1),
        mode=lax.GatherScatterMode.PROMISE_IN_BOUNDS,
    )


def spot_weights(lines, group):
    angles = len(lines)
    row = lax.broadcasted_iota(jnp.int32, (SUBLANES, LANES), 0)
    value = jnp.broadcast_to(lines[0], (SUBLANES, LANES))
    for a in range(1, angles):
        value = jnp.where(row % angles == a, jnp.broadcast_to(lines[a], (SUBLANES, LANES)), value)
    left = value >> FRACTION_BITS
    lane, level = left & (LANES - 1), left >> 7
    right_w = (value & (2**FRACTION_BITS - 1)).astype(jnp.float32) * jnp.float32(2.0**-FRACTION_BITS)
    left_w = 1.0 - right_w
    masks = [level == (row + at) // angles for at in range(0, group, SUBLANES)]

    def stack(parts):
        return jnp.concatenate(parts, axis=0)

    return (
        stack([lane] * len(masks)).astype(jnp.int16),
        stack([jnp.where(m, left_w, 0.0) for m in masks]).astype(jnp.bfloat16),
        stack([jnp.where(m, right_w, 0.0) for m in masks]).astype(jnp.bfloat16),
    )


def fold(value):
    value = value.astype(jnp.float32)
    total = value[:SUBLANES]
    for at in range(SUBLANES, value.shape[0], SUBLANES):
        total = total + value[at : at + SUBLANES]
    return total


def spot_sums(tables, lines, slices, sums):
    group = tables.shape[1] // slices
    index, left_w, right_w = spot_weights(lines, group)
    result = []
    for s in range(slices):
        at = slice(s * group, (s + 1) * group)
        value = fold(left_w * pick(tables[0, at, :], index) + right_w * pick(tables[1, at, :], index))
        result.append(value if sums is None else sums[s] + value)
    return result


def add_rows(sums):
    row = lax.broadcasted_iota(jnp.int32, (SUBLANES, LANES), 0)

    def join(a, b, shift):
        low = (row & shift) == 0
        return jnp.where(low, a + pltpu.roll(a, SUBLANES - shift, 0), b + pltpu.roll(b, shift, 0))

    done = []
    for start in range(0, len(sums), SUBLANES):
        part = sums[start : start + SUBLANES]
        part = part + [jnp.zeros_like(part[0])] * (SUBLANES - len(part))
        for shift in (4, 2, 1):
            part = [join(part[i], part[i + shift], shift) for i in range(shift)]
        done.append(part[0])
    done = done[0] if len(done) == 1 else jnp.concatenate(done, axis=0)
    return done[: len(sums)]


def kernel(
    groups, halves, row_share, sino_hbm, coord_hbm, out, sino, strip, rows_f, tables_f, tables,
    raw, coords, stage, early, send, recv, local_sem, t_send, t_recv, c_send, c_recv, p_send, p_recv, lower_sem, next_sem, upper_sem,
):
    me, half = lax.axis_index("ang"), lax.axis_index("sl")
    core = lax.rem(me, CORES)
    mate = me + 1 - 2 * core
    slices, angles, bins = sino.shape
    tiles, per_tile, width = raw.shape[1:]
    columns = width // CORES
    share = tiles * per_tile // row_share
    across = columns // LANES
    per_step = per_tile // row_share
    part_rows = per_tile // PARTS

    def block(t, tile, part, k):
        return ((t * tiles + tile) * PARTS + part) * CORES + k

    get_sino = pltpu.make_async_copy(sino_hbm, sino, local_sem.at[0])
    get_coords = pltpu.make_async_copy(coord_hbm, raw, local_sem.at[1])
    get_sino.start()
    get_coords.start()

    quad = 2 * CORES
    place, places = me // quad, groups // quad
    barrier = pltpu.get_barrier_semaphore()

    def signal(sem, ang, sl):
        pl.semaphore_signal(sem, inc=1, device_id={"ang": ang, "sl": sl}, device_id_type=MESH)

    for t in range(1, halves):
        signal(barrier, me, lax.rem(half + t, halves))
        signal(barrier, mate, lax.rem(half + t, halves))
    for k in range(1, quad):
        signal(barrier, place * quad + lax.rem(me + k, quad), half)
    has_lower, has_upper = place > 0, place < places - 1

    @pl.when(has_lower)
    def _():
        signal(barrier, me - quad, half)

    @pl.when(has_upper)
    def _():
        for k in range(quad):
            signal(barrier, (place + 1) * quad + k, half)

    build_strip(strip, bins)
    get_sino.wait()
    filter_rows(sino, strip, rows_f, 2 * LANES)
    build_tables(rows_f, tables_f, slices, angles)
    for v in range(2):
        tables[core, v] = tables_f[v].astype(jnp.bfloat16)
    get_coords.wait()
    own_side, mate_side = (
        pl.ds(pl.multiple_of(c * columns, LANES), columns) for c in (core, 1 - core)
    )
    for tile in range(tiles):
        for part in range(PARTS):
            at = slice(part * part_rows, (part + 1) * part_rows)
            coords[block(half, tile, part, core)] = jnp.concatenate(
                [raw[a, tile, at, own_side] for a in range(angles)], axis=0
            )
            stage[tile * PARTS + part] = jnp.concatenate(
                [raw[a, tile, at, mate_side] for a in range(angles)], axis=0
            )
    beside = quad * has_lower.astype(jnp.int32) + has_upper.astype(jnp.int32)
    pl.semaphore_wait(barrier, quad - 1 + CORES * (halves - 1) + beside)

    @pl.when(jnp.logical_and(place == 1, has_upper))
    def _():
        signal(lower_sem, me + quad, half)

    @pl.when(has_lower)
    def _():
        signal(next_sem, me - quad, half)

    def remote(source, target, send_sem, recv_sem, ang, sl):
        return pltpu.make_async_remote_copy(
            src_ref=source, dst_ref=target, send_sem=send_sem, recv_sem=recv_sem,
            device_id={"ang": ang, "sl": sl}, device_id_type=MESH,
        )

    def coord_copy(tile, part, source, ang, t):
        return remote(
            source, coords.at[block(half, tile, part, core)], c_send, c_recv.at[half, tile, part],
            ang, lax.rem(half + t, halves),
        )

    def start_sides(tile, part):
        for t in range(1, halves):
            mine = coords.at[block(half, tile, part, core)]
            coord_copy(tile, part, mine, me, t).start()
            coord_copy(tile, part, stage.at[tile * PARTS + part], mate, t).start()

    chunks = [(tile, part) for tile in range(tiles) for part in range(PARTS)]
    start_sides(*chunks[0])
    for tile, part in chunks:
        coord_copy(tile, part, stage.at[tile * PARTS + part], mate, 0).start()
    mate_tables = remote(tables.at[core], tables.at[core], t_send, t_recv, mate, half)
    mate_tables.start()

    def lines(t, k, tile, r, x):
        part, at = r // part_rows, r % part_rows
        return [
            coords[
                block(t, tile, part, k), a * part_rows + at : a * part_rows + at + 1,
                x * LANES : (x + 1) * LANES,
            ]
            for a in range(angles)
        ]

    spots = [(r, x) for r in range(per_tile) for x in range(across)]

    def own_angles(tile, carry):
        for r, x in spots:
            sums = spot_sums(tables.at[core], lines(half, core, tile, r, x), slices, None)
            for s in range(slices):
                early[tile, r * across + x, s] = sums[s]

        @pl.when(tile == 0)
        def _():
            start_sides(*chunks[1])

        @pl.when(jnp.logical_and(tile == 0, jnp.logical_and(place > 1, has_upper)))
        def _():
            pl.semaphore_wait(lower_sem, 1)
            signal(lower_sem, me + quad, half)

        return carry

    lax.fori_loop(0, tiles, own_angles, 0)
    for chunk in chunks[2:3]:
        start_sides(*chunk)

    def part_copy(owner):
        return remote(send.at[owner], recv.at[me], p_send, p_recv, owner, half)

    steps = halves * tiles
    beyond = places - 1 - place
    near_step = jnp.where(place == 0, tiles - 1, 0)
    far_step = jnp.where(beyond <= 2, min(tiles, steps - 1), steps - 1)
    has_far = beyond > 1

    def step_owner(step, o):
        t, tile = step // tiles, lax.rem(step, tiles)
        return lax.rem(half + t, halves) * share + tile * per_step + o

    per_part = per_step // PARTS
    parts = [range(part * per_part, (part + 1) * per_part) for part in range(PARTS)]

    def keep(step, owners, done):
        for o in owners:
            value = jnp.concatenate(
                [
                    jnp.concatenate([done[o * row_share + i, x] for x in range(across)], axis=1)
                    for i in range(row_share)
                ],
                axis=0,
            )
            send[step_owner(step, o)] = value.astype(jnp.bfloat16)

    def deliver(step, owners, wanted):
        for o in owners:
            owner = step_owner(step, o)

            @pl.when(jnp.logical_and(owner != me, wanted(owner // quad)))
            def _():
                part_copy(owner).start()

    def tell_lower():
        @pl.when(has_lower)
        def _():
            signal(upper_sem, me - quad, half)

    def late(now, step, wanted):
        def one_step(earlier, carry):
            deliver(earlier, range(per_step), wanted)
            return carry

        lax.fori_loop(0, jnp.where(now, step + 1, 0), one_step, 0)

    def hear(step):
        now = jnp.logical_and(near_step == step, has_upper)

        @pl.when(now)
        def _():
            pl.semaphore_wait(next_sem, 1)

            @pl.when(jnp.logical_not(has_far))
            def _():
                tell_lower()

        late(now, step, lambda to: to == place + 1)
        now = jnp.logical_and(far_step == step, has_far)

        @pl.when(now)
        def _():
            pl.semaphore_wait(upper_sem, 1)
            tell_lower()

        late(now, step, lambda to: to > place + 1)

    def hear_lower(step):
        @pl.when(jnp.logical_and(step == 0, jnp.logical_and(place > 1, jnp.logical_not(has_upper))))
        def _():
            pl.semaphore_wait(lower_sem, 1)

    def run_step(step, arrived, sums_of, first):
        for part, owners in enumerate(parts):
            arrived(part)
            done = {}
            for o in owners:
                for i in range(row_share):
                    for x in range(across):
                        r = o * row_share + i
                        done[r, x] = add_rows(sums_of(r, x))
            keep(step, owners, done)
            if first and part == 0:
                hear_lower(step)
            heard = place + (near_step < step).astype(jnp.int32)
            heard = jnp.where(far_step < step, places, heard)
            deliver(step, owners, lambda to: to <= heard)

    mate_tables.wait_recv()
    for chunk in chunks[3:]:
        start_sides(*chunk)

    def coords_arrived(t, tile, part, count):
        at = pl.ds(block(t, tile, part, 0), count)
        pltpu.make_async_copy(coords.at[at], coords.at[at], c_recv.at[t, tile, part]).wait()

    def mate_angles(tile, carry):
        def arrived(part):
            coords_arrived(half, tile, part, 1)

        def sums_of(r, x):
            sums = [early[tile, r * across + x, s] for s in range(slices)]
            return spot_sums(
                tables.at[1 - core], lines(half, 1 - core, tile, r, x), slices, sums
            )

        run_step(tile, arrived, sums_of, True)
        hear(tile)
        return carry

    lax.fori_loop(0, tiles, mate_angles, 0)

    def all_angles(step, carry):
        side, tile = lax.rem(half + step // tiles, halves), lax.rem(step, tiles)

        def arrived(part):
            coords_arrived(side, tile, part, CORES)

        def sums_of(r, x):
            sums = None
            for k in range(CORES):
                sums = spot_sums(tables.at[k], lines(side, k, tile, r, x), slices, sums)
            return sums

        run_step(step, arrived, sums_of, False)
        hear(step)
        return carry

    lax.fori_loop(tiles, steps, all_angles, 0)

    others = pl.ds(0, groups - 1)
    everyone = remote(send.at[others], recv.at[others], p_send, p_recv, mate, half)
    everyone.wait_recv()
    recv[me] = send[me]
    totals = [None] * CORES
    for source in range(groups):
        value = recv[source].astype(jnp.float32)
        c = source % CORES
        totals[c] = value if totals[c] is None else totals[c] + value
    scale = jnp.float32(math.pi / (angles * groups))
    for c in range(CORES):
        total = totals[c] * scale
        for i in range(row_share):
            out[i, :, c * columns : (c + 1) * columns] = total[i * slices : (i + 1) * slices]
    mate_tables.wait_send()
    given = coords.at[pl.ds(0, len(chunks) * (1 + CORES * (halves - 1)))]
    remote(given, given, c_send, c_recv.at[0, 0, 0], mate, half).wait_send()
    everyone.wait_send()


def shards(sinogram, detector_coord):
    slices, angles, bins = sinogram.shape
    local_rows, width = detector_coord.shape[1:]
    groups, halves = lax.axis_size("ang"), lax.axis_size("sl")
    row_share = local_rows * halves // groups
    tiles, columns = local_rows // SUBLANES, width // CORES
    group = bins // LANES * angles
    coords = detector_coord.reshape(angles, tiles, SUBLANES, width)
    block = (angles * SUBLANES // PARTS, columns)
    message = (groups, row_share * slices, columns)
    spots = SUBLANES * columns // LANES
    dma = pltpu.SemaphoreType.DMA
    return pl.pallas_call(
        functools.partial(kernel, groups, halves, row_share),
        out_shape=pltpu.VMEM((row_share, slices, width), jnp.float32),
        in_specs=[pl.BlockSpec(memory_space=pl.ANY)] * 2,
        out_specs=pl.BlockSpec(memory_space=pltpu.VMEM),
        scratch_shapes=[
            pltpu.VMEM(sinogram.shape, sinogram.dtype),
            pltpu.VMEM((2 * bins - LANES, LANES), jnp.bfloat16),
            pltpu.VMEM((slices * group, LANES), jnp.float32),
            pltpu.VMEM((2, slices * group, LANES), jnp.float32),
            pltpu.VMEM((CORES, 2, slices * group, LANES), jnp.bfloat16),
            pltpu.VMEM(coords.shape, jnp.int32),
            pltpu.VMEM((halves * tiles * PARTS * CORES,) + block, jnp.int32),
            pltpu.VMEM((tiles * PARTS,) + block, jnp.int32),
            pltpu.VMEM((tiles, spots, slices, SUBLANES, LANES), jnp.float32),
            pltpu.VMEM(message, jnp.bfloat16),
            pltpu.VMEM(message, jnp.bfloat16),
            dma((2,)),
            dma(()),
            dma(()),
            dma(()),
            dma((halves, tiles, PARTS)),
            dma(()),
            dma(()),
            pltpu.SemaphoreType.REGULAR,
            pltpu.SemaphoreType.REGULAR,
            pltpu.SemaphoreType.REGULAR,
        ],
        compiler_params=pltpu.CompilerParams(collective_id=0, has_side_effects=True),
    )(sinogram, coords)


def solution(mesh):
    in_specs = (P("sl", "ang", None), P("ang", "sl", None))
    out_specs = P("ang", "sl", None)
    return jax.shard_map(shards, mesh=mesh, in_specs=in_specs, out_specs=out_specs, check_vma=False)
```

```python
import functools
import math

import jax
import jax.numpy as jnp
from jax import lax
from jax.experimental import pallas as pl
from jax.experimental.pallas import tpu as pltpu
from jax.sharding import PartitionSpec as P

LANES = 128
SUBLANES = 8
CORES = 2
PARTS = 2
FRACTION_BITS = 20
MESH = pl.DeviceIdType.MESH
ALONG_LANES = lax.GatherDimensionNumbers(
    offset_dims=(),
    collapsed_slice_dims=(1,),
    start_index_map=(1,),
    operand_batching_dims=(0,),
    start_indices_batching_dims=(0,),
)


def build_strip(strip, bins):
    row = lax.broadcasted_iota(jnp.int32, strip.shape, 0)
    lane = lax.broadcasted_iota(jnp.int32, strip.shape, 1)
    offset = lane - row + (bins - LANES)
    wide = offset.astype(jnp.float32)
    square = jnp.maximum(wide * wide, jnp.float32(1.0))
    odd = jnp.where((offset & 1) != 0, jnp.float32(-1.0 / math.pi**2) / square, jnp.float32(0.0))
    strip[...] = jnp.where(offset == 0, jnp.float32(0.25), odd).astype(jnp.bfloat16)


def filter_rows(sino, strip, rows_f, size):
    slices, angles, bins = sino.shape
    rows, count = slices * angles, bins // size
    blocks = [sino[:, :, i * size : (i + 1) * size].reshape(rows, size) for i in range(count)]
    totals = [None] * count
    for d in range(1 - count, count):
        inner = [i for i in range(count) if 0 <= i + d < count]
        first = bins - LANES - size * d
        right = jnp.concatenate(
            [strip[first - u : first - u + size, :] for u in range(0, size, LANES)], axis=1
        )
        left = jnp.concatenate([blocks[i] for i in inner], axis=0)
        part = jnp.dot(left, right, preferred_element_type=jnp.float32)
        for at, i in enumerate(inner):
            piece = part[at * rows : (at + 1) * rows]
            totals[i + d] = piece if totals[i + d] is None else totals[i + d] + piece
    for j, total in enumerate(totals):
        total = total.astype(jnp.bfloat16).astype(jnp.float32)
        for u in range(0, size, LANES):
            at = (j * size + u) // LANES * rows
            rows_f[at : at + rows, :] = total[:, u : u + LANES]


def build_tables(rows_f, tables_f, slices, angles):
    levels = rows_f.shape[0] // (slices * angles)
    bins = levels * LANES
    for a in range(angles):
        starts = [level * slices * angles + a for level in range(levels)]
        here = jnp.concatenate(
            [rows_f[pl.ds(at, slices, stride=angles), :] for at in starts], axis=1
        )
        following = pltpu.roll(here, bins - 1, 1)
        for v, value in enumerate((here, following)):
            for level in range(levels):
                at = pl.ds(level * angles + a, slices, stride=levels * angles)
                tables_f[v, at, :] = value[:, level * LANES : (level + 1) * LANES]


def pick(table, index):
    return lax.gather(
        table, index[..., None], ALONG_LANES, (1, 1),
        mode=lax.GatherScatterMode.PROMISE_IN_BOUNDS,
    )


def spot_weights(lines, group):
    angles = len(lines)
    row = lax.broadcasted_iota(jnp.int32, (SUBLANES, LANES), 0)
    value = jnp.broadcast_to(lines[0], (SUBLANES, LANES))
    for a in range(1, angles):
        value = jnp.where(row % angles == a, jnp.broadcast_to(lines[a], (SUBLANES, LANES)), value)
    left = value >> FRACTION_BITS
    lane, level = left & (LANES - 1), left >> 7
    right_w = (value & (2**FRACTION_BITS - 1)).astype(jnp.float32) * jnp.float32(2.0**-FRACTION_BITS)
    left_w = 1.0 - right_w
    masks = [level == (row + at) // angles for at in range(0, group, SUBLANES)]

    def stack(parts):
        return jnp.concatenate(parts, axis=0)

    return (
        stack([lane] * len(masks)).astype(jnp.int16),
        stack([jnp.where(m, left_w, 0.0) for m in masks]).astype(jnp.bfloat16),
        stack([jnp.where(m, right_w, 0.0) for m in masks]).astype(jnp.bfloat16),
    )


def fold(value):
    value = value.astype(jnp.float32)
    total = value[:SUBLANES]
    for at in range(SUBLANES, value.shape[0], SUBLANES):
        total = total + value[at : at + SUBLANES]
    return total


def spot_sums(tables, lines, slices, sums):
    group = tables.shape[1] // slices
    index, left_w, right_w = spot_weights(lines, group)
    result = []
    for s in range(slices):
        at = slice(s * group, (s + 1) * group)
        value = fold(left_w * pick(tables[0, at, :], index) + right_w * pick(tables[1, at, :], index))
        result.append(value if sums is None else sums[s] + value)
    return result


def add_rows(sums):
    row = lax.broadcasted_iota(jnp.int32, (SUBLANES, LANES), 0)

    def join(a, b, shift):
        low = (row & shift) == 0
        return jnp.where(low, a + pltpu.roll(a, SUBLANES - shift, 0), b + pltpu.roll(b, shift, 0))

    done = []
    for start in range(0, len(sums), SUBLANES):
        part = sums[start : start + SUBLANES]
        part = part + [jnp.zeros_like(part[0])] * (SUBLANES - len(part))
        for shift in (4, 2, 1):
            part = [join(part[i], part[i + shift], shift) for i in range(shift)]
        done.append(part[0])
    done = done[0] if len(done) == 1 else jnp.concatenate(done, axis=0)
    return done[: len(sums)]


def kernel(
    groups, halves, row_share, sino_hbm, coord_hbm, out, sino, strip, rows_f, tables_f, tables,
    raw, coords, stage, early, send, recv, local_sem, t_send, t_recv, c_send, c_recv, p_send, p_recv, lower_sem, next_sem, upper_sem,
):
    me, half = lax.axis_index("ang"), lax.axis_index("sl")
    core = lax.rem(me, CORES)
    mate = me + 1 - 2 * core
    slices, angles, bins = sino.shape
    tiles, per_tile, width = raw.shape[1:]
    columns = width // CORES
    share = tiles * per_tile // row_share
    across = columns // LANES
    per_step = per_tile // row_share
    part_rows = per_tile // PARTS

    def block(t, tile, part, k):
        return ((t * tiles + tile) * PARTS + part) * CORES + k

    get_sino = pltpu.make_async_copy(sino_hbm, sino, local_sem.at[0])
    get_coords = pltpu.make_async_copy(coord_hbm, raw, local_sem.at[1])
    get_sino.start()
    get_coords.start()

    quad = 2 * CORES
    place, places = me // quad, groups // quad
    barrier = pltpu.get_barrier_semaphore()

    def signal(sem, ang, sl):
        pl.semaphore_signal(sem, inc=1, device_id={"ang": ang, "sl": sl}, device_id_type=MESH)

    for t in range(1, halves):
        signal(barrier, me, lax.rem(half + t, halves))
        signal(barrier, mate, lax.rem(half + t, halves))
    for k in range(1, quad):
        signal(barrier, place * quad + lax.rem(me + k, quad), half)
    has_lower, has_upper = place > 0, place < places - 1

    @pl.when(has_lower)
    def _():
        signal(barrier, me - quad, half)

    @pl.when(has_upper)
    def _():
        for k in range(quad):
            signal(barrier, (place + 1) * quad + k, half)

    build_strip(strip, bins)
    get_sino.wait()
    filter_rows(sino, strip, rows_f, 2 * LANES)
    build_tables(rows_f, tables_f, slices, angles)
    for v in range(2):
        tables[core, v] = tables_f[v].astype(jnp.bfloat16)
    get_coords.wait()
    own_side, mate_side = (
        pl.ds(pl.multiple_of(c * columns, LANES), columns) for c in (core, 1 - core)
    )
    for tile in range(tiles):
        for part in range(PARTS):
            at = slice(part * part_rows, (part + 1) * part_rows)
            coords[block(half, tile, part, core)] = jnp.concatenate(
                [raw[a, tile, at, own_side] for a in range(angles)], axis=0
            )
            stage[tile * PARTS + part] = jnp.concatenate(
                [raw[a, tile, at, mate_side] for a in range(angles)], axis=0
            )
    beside = quad * has_lower.astype(jnp.int32) + has_upper.astype(jnp.int32)
    pl.semaphore_wait(barrier, quad - 1 + CORES * (halves - 1) + beside)

    @pl.when(jnp.logical_and(place == 1, has_upper))
    def _():
        signal(lower_sem, me + quad, half)

    @pl.when(has_lower)
    def _():
        signal(next_sem, me - quad, half)

    def remote(source, target, send_sem, recv_sem, ang, sl):
        return pltpu.make_async_remote_copy(
            src_ref=source, dst_ref=target, send_sem=send_sem, recv_sem=recv_sem,
            device_id={"ang": ang, "sl": sl}, device_id_type=MESH,
        )

    def coord_copy(tile, part, source, ang, t):
        return remote(
            source, coords.at[block(half, tile, part, core)], c_send, c_recv.at[half, tile, part],
            ang, lax.rem(half + t, halves),
        )

    def start_sides(tile, part):
        for t in range(1, halves):
            mine = coords.at[block(half, tile, part, core)]
            coord_copy(tile, part, mine, me, t).start()
            coord_copy(tile, part, stage.at[tile * PARTS + part], mate, t).start()

    chunks = [(tile, part) for tile in range(tiles) for part in range(PARTS)]
    start_sides(*chunks[0])
    for tile, part in chunks:
        coord_copy(tile, part, stage.at[tile * PARTS + part], mate, 0).start()
    mate_tables = remote(tables.at[core], tables.at[core], t_send, t_recv, mate, half)
    mate_tables.start()

    def lines(t, k, tile, r, x):
        part, at = r // part_rows, r % part_rows
        return [
            coords[
                block(t, tile, part, k), a * part_rows + at : a * part_rows + at + 1,
                x * LANES : (x + 1) * LANES,
            ]
            for a in range(angles)
        ]

    spots = [(r, x) for r in range(per_tile) for x in range(across)]

    def own_angles(tile, carry):
        for r, x in spots:
            sums = spot_sums(tables.at[core], lines(half, core, tile, r, x), slices, None)
            for s in range(slices):
                early[tile, r * across + x, s] = sums[s]

        @pl.when(tile == 0)
        def _():
            start_sides(*chunks[1])

        @pl.when(jnp.logical_and(tile == 0, jnp.logical_and(place > 1, has_upper)))
        def _():
            pl.semaphore_wait(lower_sem, 1)
            signal(lower_sem, me + quad, half)

        return carry

    lax.fori_loop(0, tiles, own_angles, 0)
    for chunk in chunks[2:3]:
        start_sides(*chunk)

    def part_copy(owner):
        return remote(send.at[owner], recv.at[me], p_send, p_recv, owner, half)

    steps = halves * tiles
    beyond = places - 1 - place
    near_step = jnp.where(place == 0, tiles - 1, 0)
    far_step = jnp.where(beyond <= 2, min(tiles, steps - 1), steps - 1)
    has_far = beyond > 1

    def step_owner(step, o):
        t, tile = step // tiles, lax.rem(step, tiles)
        return lax.rem(half + t, halves) * share + tile * per_step + o

    per_part = per_step // PARTS
    parts = [range(part * per_part, (part + 1) * per_part) for part in range(PARTS)]

    def keep(step, owners, done):
        for o in owners:
            value = jnp.concatenate(
                [
                    jnp.concatenate([done[o * row_share + i, x] for x in range(across)], axis=1)
                    for i in range(row_share)
                ],
                axis=0,
            )
            send[step_owner(step, o)] = value.astype(jnp.bfloat16)

    def deliver(step, owners, wanted):
        for o in owners:
            owner = step_owner(step, o)

            @pl.when(jnp.logical_and(owner != me, wanted(owner // quad)))
            def _():
                part_copy(owner).start()

    def tell_lower():
        @pl.when(has_lower)
        def _():
            signal(upper_sem, me - quad, half)

    def late(now, step, wanted):
        def one_step(earlier, carry):
            deliver(step - earlier, range(per_step), wanted)
            return carry

        lax.fori_loop(0, jnp.where(now, step + 1, 0), one_step, 0)

    def hear(step):
        now = jnp.logical_and(near_step == step, has_upper)

        @pl.when(now)
        def _():
            pl.semaphore_wait(next_sem, 1)

            @pl.when(jnp.logical_not(has_far))
            def _():
                tell_lower()

        late(now, step, lambda to: to == place + 1)
        now = jnp.logical_and(far_step == step, has_far)

        @pl.when(now)
        def _():
            pl.semaphore_wait(upper_sem, 1)
            tell_lower()

        late(now, step, lambda to: to > place + 1)

    def hear_lower(step):
        @pl.when(jnp.logical_and(step == 0, jnp.logical_and(place > 1, jnp.logical_not(has_upper))))
        def _():
            pl.semaphore_wait(lower_sem, 1)

    def run_step(step, arrived, sums_of, first):
        for part, owners in enumerate(parts):
            arrived(part)
            done = {}
            for o in owners:
                for i in range(row_share):
                    for x in range(across):
                        r = o * row_share + i
                        done[r, x] = add_rows(sums_of(r, x))
            keep(step, owners, done)
            if first and part == 0:
                hear_lower(step)
            heard = place + (near_step < step).astype(jnp.int32)
            heard = jnp.where(far_step < step, places, heard)
            deliver(step, owners, lambda to: to <= heard)

    mate_tables.wait_recv()
    for chunk in chunks[3:]:
        start_sides(*chunk)

    def coords_arrived(t, tile, part, count):
        at = pl.ds(block(t, tile, part, 0), count)
        pltpu.make_async_copy(coords.at[at], coords.at[at], c_recv.at[t, tile, part]).wait()

    def mate_angles(tile, carry):
        def arrived(part):
            coords_arrived(half, tile, part, 1)

        def sums_of(r, x):
            sums = [early[tile, r * across + x, s] for s in range(slices)]
            return spot_sums(
                tables.at[1 - core], lines(half, 1 - core, tile, r, x), slices, sums
            )

        run_step(tile, arrived, sums_of, True)
        hear(tile)
        return carry

    lax.fori_loop(0, tiles, mate_angles, 0)

    def all_angles(step, carry):
        side, tile = lax.rem(half + step // tiles, halves), lax.rem(step, tiles)

        def arrived(part):
            coords_arrived(side, tile, part, CORES)

        def sums_of(r, x):
            sums = None
            for k in range(CORES):
                sums = spot_sums(tables.at[k], lines(side, k, tile, r, x), slices, sums)
            return sums

        run_step(step, arrived, sums_of, False)
        hear(step)
        return carry

    lax.fori_loop(tiles, steps, all_angles, 0)

    others = pl.ds(0, groups - 1)
    everyone = remote(send.at[others], recv.at[others], p_send, p_recv, mate, half)
    everyone.wait_recv()
    recv[me] = send[me]
    totals = [None] * CORES
    for source in range(groups):
        value = recv[source].astype(jnp.float32)
        c = source % CORES
        totals[c] = value if totals[c] is None else totals[c] + value
    scale = jnp.float32(math.pi / (angles * groups))
    for c in range(CORES):
        total = totals[c] * scale
        for i in range(row_share):
            out[i, :, c * columns : (c + 1) * columns] = total[i * slices : (i + 1) * slices]
    mate_tables.wait_send()
    given = coords.at[pl.ds(0, len(chunks) * (1 + CORES * (halves - 1)))]
    remote(given, given, c_send, c_recv.at[0, 0, 0], mate, half).wait_send()
    everyone.wait_send()


def shards(sinogram, detector_coord):
    slices, angles, bins = sinogram.shape
    local_rows, width = detector_coord.shape[1:]
    groups, halves = lax.axis_size("ang"), lax.axis_size("sl")
    row_share = local_rows * halves // groups
    tiles, columns = local_rows // SUBLANES, width // CORES
    group = bins // LANES * angles
    coords = detector_coord.reshape(angles, tiles, SUBLANES, width)
    block = (angles * SUBLANES // PARTS, columns)
    message = (groups, row_share * slices, columns)
    spots = SUBLANES * columns // LANES
    dma = pltpu.SemaphoreType.DMA
    return pl.pallas_call(
        functools.partial(kernel, groups, halves, row_share),
        out_shape=pltpu.VMEM((row_share, slices, width), jnp.float32),
        in_specs=[pl.BlockSpec(memory_space=pl.ANY)] * 2,
        out_specs=pl.BlockSpec(memory_space=pltpu.VMEM),
        scratch_shapes=[
            pltpu.VMEM(sinogram.shape, sinogram.dtype),
            pltpu.VMEM((2 * bins - LANES, LANES), jnp.bfloat16),
            pltpu.VMEM((slices * group, LANES), jnp.float32),
            pltpu.VMEM((2, slices * group, LANES), jnp.float32),
            pltpu.VMEM((CORES, 2, slices * group, LANES), jnp.bfloat16),
            pltpu.VMEM(coords.shape, jnp.int32),
            pltpu.VMEM((halves * tiles * PARTS * CORES,) + block, jnp.int32),
            pltpu.VMEM((tiles * PARTS,) + block, jnp.int32),
            pltpu.VMEM((tiles, spots, slices, SUBLANES, LANES), jnp.float32),
            pltpu.VMEM(message, jnp.bfloat16),
            pltpu.VMEM(message, jnp.bfloat16),
            dma((2,)),
            dma(()),
            dma(()),
            dma(()),
            dma((halves, tiles, PARTS)),
            dma(()),
            dma(()),
            pltpu.SemaphoreType.REGULAR,
            pltpu.SemaphoreType.REGULAR,
            pltpu.SemaphoreType.REGULAR,
        ],
        compiler_params=pltpu.CompilerParams(collective_id=0, has_side_effects=True),
    )(sinogram, coords)


def solution(mesh):
    in_specs = (P("sl", "ang", None), P("ang", "sl", None))
    out_specs = P("ang", "sl", None)
    return jax.shard_map(shards, mesh=mesh, in_specs=in_specs, out_specs=out_specs, check_vma=False)
```

```python
import functools
import math

import jax
import jax.numpy as jnp
from jax import lax
from jax.experimental import pallas as pl
from jax.experimental.pallas import tpu as pltpu
from jax.sharding import PartitionSpec as P

LANES = 128
SUBLANES = 8
CORES = 2
PARTS = 2
FRACTION_BITS = 20
MESH = pl.DeviceIdType.MESH
ALONG_LANES = lax.GatherDimensionNumbers(
    offset_dims=(),
    collapsed_slice_dims=(1,),
    start_index_map=(1,),
    operand_batching_dims=(0,),
    start_indices_batching_dims=(0,),
)


def build_strip(strip, bins):
    row = lax.broadcasted_iota(jnp.int32, strip.shape, 0)
    lane = lax.broadcasted_iota(jnp.int32, strip.shape, 1)
    offset = lane - row + (bins - LANES)
    wide = offset.astype(jnp.float32)
    square = jnp.maximum(wide * wide, jnp.float32(1.0))
    odd = jnp.where((offset & 1) != 0, jnp.float32(-1.0 / math.pi**2) / square, jnp.float32(0.0))
    strip[...] = jnp.where(offset == 0, jnp.float32(0.25), odd).astype(jnp.bfloat16)


def filter_rows(sino, strip, rows_f, size):
    slices, angles, bins = sino.shape
    rows, count = slices * angles, bins // size
    blocks = [sino[:, :, i * size : (i + 1) * size].reshape(rows, size) for i in range(count)]
    totals = [None] * count
    for d in range(1 - count, count):
        inner = [i for i in range(count) if 0 <= i + d < count]
        first = bins - LANES - size * d
        right = jnp.concatenate(
            [strip[first - u : first - u + size, :] for u in range(0, size, LANES)], axis=1
        )
        left = jnp.concatenate([blocks[i] for i in inner], axis=0)
        part = jnp.dot(left, right, preferred_element_type=jnp.float32)
        for at, i in enumerate(inner):
            piece = part[at * rows : (at + 1) * rows]
            totals[i + d] = piece if totals[i + d] is None else totals[i + d] + piece
    for j, total in enumerate(totals):
        total = total.astype(jnp.bfloat16).astype(jnp.float32)
        for u in range(0, size, LANES):
            at = (j * size + u) // LANES * rows
            rows_f[at : at + rows, :] = total[:, u : u + LANES]


def build_tables(rows_f, tables_f, slices, angles):
    levels = rows_f.shape[0] // (slices * angles)
    bins = levels * LANES
    for a in range(angles):
        starts = [level * slices * angles + a for level in range(levels)]
        here = jnp.concatenate(
            [rows_f[pl.ds(at, slices, stride=angles), :] for at in starts], axis=1
        )
        following = pltpu.roll(here, bins - 1, 1)
        for v, value in enumerate((here, following)):
            for level in range(levels):
                at = pl.ds(level * angles + a, slices, stride=levels * angles)
                tables_f[v, at, :] = value[:, level * LANES : (level + 1) * LANES]


def pick(table, index):
    return lax.gather(
        table, index[..., None], ALONG_LANES, (1, 1),
        mode=lax.GatherScatterMode.PROMISE_IN_BOUNDS,
    )


def spot_weights(lines, group):
    angles = len(lines)
    row = lax.broadcasted_iota(jnp.int32, (SUBLANES, LANES), 0)
    value = jnp.broadcast_to(lines[0], (SUBLANES, LANES))
    for a in range(1, angles):
        value = jnp.where(row % angles == a, jnp.broadcast_to(lines[a], (SUBLANES, LANES)), value)
    left = value >> FRACTION_BITS
    lane, level = left & (LANES - 1), left >> 7
    right_w = (value & (2**FRACTION_BITS - 1)).astype(jnp.float32) * jnp.float32(2.0**-FRACTION_BITS)
    left_w = 1.0 - right_w
    masks = [level == (row + at) // angles for at in range(0, group, SUBLANES)]

    def stack(parts):
        return jnp.concatenate(parts, axis=0)

    return (
        stack([lane] * len(masks)).astype(jnp.int16),
        stack([jnp.where(m, left_w, 0.0) for m in masks]).astype(jnp.bfloat16),
        stack([jnp.where(m, right_w, 0.0) for m in masks]).astype(jnp.bfloat16),
    )


def fold(value):
    value = value.astype(jnp.float32)
    total = value[:SUBLANES]
    for at in range(SUBLANES, value.shape[0], SUBLANES):
        total = total + value[at : at + SUBLANES]
    return total


def spot_sums(tables, lines, slices, sums):
    group = tables.shape[1] // slices
    index, left_w, right_w = spot_weights(lines, group)
    result = []
    for s in range(slices):
        at = slice(s * group, (s + 1) * group)
        value = fold(left_w * pick(tables[0, at, :], index) + right_w * pick(tables[1, at, :], index))
        result.append(value if sums is None else sums[s] + value)
    return result


def add_rows(sums):
    row = lax.broadcasted_iota(jnp.int32, (SUBLANES, LANES), 0)

    def join(a, b, shift):
        low = (row & shift) == 0
        return jnp.where(low, a + pltpu.roll(a, SUBLANES - shift, 0), b + pltpu.roll(b, shift, 0))

    done = []
    for start in range(0, len(sums), SUBLANES):
        part = sums[start : start + SUBLANES]
        part = part + [jnp.zeros_like(part[0])] * (SUBLANES - len(part))
        for shift in (4, 2, 1):
            part = [join(part[i], part[i + shift], shift) for i in range(shift)]
        done.append(part[0])
    done = done[0] if len(done) == 1 else jnp.concatenate(done, axis=0)
    return done[: len(sums)]


def kernel(
    groups, halves, row_share, sino_hbm, coord_hbm, out, sino, strip, rows_f, tables_f, tables,
    raw, coords, stage, early, send, recv, local_sem, t_send, t_recv, c_send, c_recv, p_send, p_recv, lower_sem, next_sem, upper_sem,
):
    me, half = lax.axis_index("ang"), lax.axis_index("sl")
    core = lax.rem(me, CORES)
    mate = me + 1 - 2 * core
    slices, angles, bins = sino.shape
    tiles, per_tile, width = raw.shape[1:]
    columns = width // CORES
    share = tiles * per_tile // row_share
    across = columns // LANES
    per_step = per_tile // row_share
    part_rows = per_tile // PARTS

    def block(t, tile, part, k):
        return ((t * tiles + tile) * PARTS + part) * CORES + k

    get_sino = pltpu.make_async_copy(sino_hbm, sino, local_sem.at[0])
    get_coords = pltpu.make_async_copy(coord_hbm, raw, local_sem.at[1])
    get_sino.start()
    get_coords.start()

    quad = 2 * CORES
    place, places = me // quad, groups // quad
    barrier = pltpu.get_barrier_semaphore()

    def signal(sem, ang, sl):
        pl.semaphore_signal(sem, inc=1, device_id={"ang": ang, "sl": sl}, device_id_type=MESH)

    for t in range(1, halves):
        signal(barrier, me, lax.rem(half + t, halves))
        signal(barrier, mate, lax.rem(half + t, halves))
    for k in range(1, quad):
        signal(barrier, place * quad + lax.rem(me + k, quad), half)
    has_lower, has_upper = place > 0, place < places - 1

    @pl.when(has_lower)
    def _():
        signal(barrier, me - quad, half)

    @pl.when(has_upper)
    def _():
        for k in range(quad):
            signal(barrier, (place + 1) * quad + k, half)

    build_strip(strip, bins)
    get_sino.wait()
    filter_rows(sino, strip, rows_f, 2 * LANES)
    build_tables(rows_f, tables_f, slices, angles)
    for v in range(2):
        tables[core, v] = tables_f[v].astype(jnp.bfloat16)
    get_coords.wait()
    own_side, mate_side = (
        pl.ds(pl.multiple_of(c * columns, LANES), columns) for c in (core, 1 - core)
    )
    for tile in range(tiles):
        for part in range(PARTS):
            at = slice(part * part_rows, (part + 1) * part_rows)
            coords[block(half, tile, part, core)] = jnp.concatenate(
                [raw[a, tile, at, own_side] for a in range(angles)], axis=0
            )
            stage[tile * PARTS + part] = jnp.concatenate(
                [raw[a, tile, at, mate_side] for a in range(angles)], axis=0
            )
    beside = quad * has_lower.astype(jnp.int32) + has_upper.astype(jnp.int32)
    pl.semaphore_wait(barrier, quad - 1 + CORES * (halves - 1) + beside)

    @pl.when(jnp.logical_and(place == 1, has_upper))
    def _():
        signal(lower_sem, me + quad, half)

    @pl.when(has_lower)
    def _():
        signal(next_sem, me - quad, half)

    def remote(source, target, send_sem, recv_sem, ang, sl):
        return pltpu.make_async_remote_copy(
            src_ref=source, dst_ref=target, send_sem=send_sem, recv_sem=recv_sem,
            device_id={"ang": ang, "sl": sl}, device_id_type=MESH,
        )

    def coord_copy(tile, part, source, ang, t):
        return remote(
            source, coords.at[block(half, tile, part, core)], c_send, c_recv.at[half, tile, part],
            ang, lax.rem(half + t, halves),
        )

    def start_sides(tile, part):
        for t in range(1, halves):
            mine = coords.at[block(half, tile, part, core)]
            coord_copy(tile, part, mine, me, t).start()
            coord_copy(tile, part, stage.at[tile * PARTS + part], mate, t).start()

    chunks = [(tile, part) for tile in range(tiles) for part in range(PARTS)]
    start_sides(*chunks[0])
    for tile, part in chunks:
        coord_copy(tile, part, stage.at[tile * PARTS + part], mate, 0).start()
    mate_tables = remote(tables.at[core], tables.at[core], t_send, t_recv, mate, half)
    mate_tables.start()

    def lines(t, k, tile, r, x):
        part, at = r // part_rows, r % part_rows
        return [
            coords[
                block(t, tile, part, k), a * part_rows + at : a * part_rows + at + 1,
                x * LANES : (x + 1) * LANES,
            ]
            for a in range(angles)
        ]

    spots = [(r, x) for r in range(per_tile) for x in range(across)]

    def own_angles(tile, carry):
        for r, x in spots:
            sums = spot_sums(tables.at[core], lines(half, core, tile, r, x), slices, None)
            for s in range(slices):
                early[tile, r * across + x, s] = sums[s]

        @pl.when(tile == 0)
        def _():
            start_sides(*chunks[1])

        @pl.when(jnp.logical_and(tile == 0, jnp.logical_and(place > 1, has_upper)))
        def _():
            pl.semaphore_wait(lower_sem, 1)
            signal(lower_sem, me + quad, half)

        return carry

    lax.fori_loop(0, tiles, own_angles, 0)
    for chunk in chunks[2:3]:
        start_sides(*chunk)

    def part_copy(owner):
        return remote(send.at[owner], recv.at[me], p_send, p_recv, owner, half)

    steps = halves * tiles
    beyond = places - 1 - place
    near_step = jnp.where(place == 0, tiles - 1, 0)
    far_step = jnp.where(beyond <= 2, min(tiles, steps - 1), steps - 1)
    has_far = beyond > 1

    def step_owner(step, o):
        t, tile = step // tiles, lax.rem(step, tiles)
        return lax.rem(half + t, halves) * share + tile * per_step + o

    per_part = per_step // PARTS
    parts = [range(part * per_part, (part + 1) * per_part) for part in range(PARTS)]

    def keep(step, owners, done):
        for o in owners:
            value = jnp.concatenate(
                [
                    jnp.concatenate([done[o * row_share + i, x] for x in range(across)], axis=1)
                    for i in range(row_share)
                ],
                axis=0,
            )
            send[step_owner(step, o)] = value.astype(jnp.bfloat16)

    def deliver(step, owners, wanted):
        for o in sorted(owners, key=lambda o: o ^ 1):
            owner = step_owner(step, o)

            @pl.when(jnp.logical_and(owner != me, wanted(owner // quad)))
            def _():
                part_copy(owner).start()

    def tell_lower():
        @pl.when(has_lower)
        def _():
            signal(upper_sem, me - quad, half)

    def late(now, step, wanted):
        def one_step(earlier, carry):
            deliver(step - earlier, range(per_step), wanted)
            return carry

        lax.fori_loop(0, jnp.where(now, step + 1, 0), one_step, 0)

    def hear(step):
        now = jnp.logical_and(near_step == step, has_upper)

        @pl.when(now)
        def _():
            pl.semaphore_wait(next_sem, 1)

            @pl.when(jnp.logical_not(has_far))
            def _():
                tell_lower()

        late(now, step, lambda to: to == place + 1)
        now = jnp.logical_and(far_step == step, has_far)

        @pl.when(now)
        def _():
            pl.semaphore_wait(upper_sem, 1)
            tell_lower()

        late(now, step, lambda to: to > place + 1)

    def hear_lower(step):
        @pl.when(jnp.logical_and(step == 0, jnp.logical_and(place > 1, jnp.logical_not(has_upper))))
        def _():
            pl.semaphore_wait(lower_sem, 1)

    def run_step(step, arrived, sums_of, first):
        for part, owners in enumerate(parts):
            arrived(part)
            done = {}
            for o in owners:
                for i in range(row_share):
                    for x in range(across):
                        r = o * row_share + i
                        done[r, x] = add_rows(sums_of(r, x))
            keep(step, owners, done)
            if first and part == 0:
                hear_lower(step)
            heard = place + (near_step < step).astype(jnp.int32)
            heard = jnp.where(far_step < step, places, heard)
            deliver(step, owners, lambda to: to <= heard)

    mate_tables.wait_recv()
    for chunk in chunks[3:]:
        start_sides(*chunk)

    def coords_arrived(t, tile, part, count):
        at = pl.ds(block(t, tile, part, 0), count)
        pltpu.make_async_copy(coords.at[at], coords.at[at], c_recv.at[t, tile, part]).wait()

    def mate_angles(tile, carry):
        def arrived(part):
            coords_arrived(half, tile, part, 1)

        def sums_of(r, x):
            sums = [early[tile, r * across + x, s] for s in range(slices)]
            return spot_sums(
                tables.at[1 - core], lines(half, 1 - core, tile, r, x), slices, sums
            )

        run_step(tile, arrived, sums_of, True)
        hear(tile)
        return carry

    lax.fori_loop(0, tiles, mate_angles, 0)

    def all_angles(step, carry):
        side, tile = lax.rem(half + step // tiles, halves), lax.rem(step, tiles)

        def arrived(part):
            coords_arrived(side, tile, part, CORES)

        def sums_of(r, x):
            sums = None
            for k in range(CORES):
                sums = spot_sums(tables.at[k], lines(side, k, tile, r, x), slices, sums)
            return sums

        run_step(step, arrived, sums_of, False)
        hear(step)
        return carry

    lax.fori_loop(tiles, steps, all_angles, 0)

    others = pl.ds(0, groups - 1)
    everyone = remote(send.at[others], recv.at[others], p_send, p_recv, mate, half)
    everyone.wait_recv()
    recv[me] = send[me]
    totals = [None] * CORES
    for source in range(groups):
        value = recv[source].astype(jnp.float32)
        c = source % CORES
        totals[c] = value if totals[c] is None else totals[c] + value
    scale = jnp.float32(math.pi / (angles * groups))
    for c in range(CORES):
        total = totals[c] * scale
        for i in range(row_share):
            out[i, :, c * columns : (c + 1) * columns] = total[i * slices : (i + 1) * slices]
    mate_tables.wait_send()
    given = coords.at[pl.ds(0, len(chunks) * (1 + CORES * (halves - 1)))]
    remote(given, given, c_send, c_recv.at[0, 0, 0], mate, half).wait_send()
    everyone.wait_send()


def shards(sinogram, detector_coord):
    slices, angles, bins = sinogram.shape
    local_rows, width = detector_coord.shape[1:]
    groups, halves = lax.axis_size("ang"), lax.axis_size("sl")
    row_share = local_rows * halves // groups
    tiles, columns = local_rows // SUBLANES, width // CORES
    group = bins // LANES * angles
    coords = detector_coord.reshape(angles, tiles, SUBLANES, width)
    block = (angles * SUBLANES // PARTS, columns)
    message = (groups, row_share * slices, columns)
    spots = SUBLANES * columns // LANES
    dma = pltpu.SemaphoreType.DMA
    return pl.pallas_call(
        functools.partial(kernel, groups, halves, row_share),
        out_shape=pltpu.VMEM((row_share, slices, width), jnp.float32),
        in_specs=[pl.BlockSpec(memory_space=pl.ANY)] * 2,
        out_specs=pl.BlockSpec(memory_space=pltpu.VMEM),
        scratch_shapes=[
            pltpu.VMEM(sinogram.shape, sinogram.dtype),
            pltpu.VMEM((2 * bins - LANES, LANES), jnp.bfloat16),
            pltpu.VMEM((slices * group, LANES), jnp.float32),
            pltpu.VMEM((2, slices * group, LANES), jnp.float32),
            pltpu.VMEM((CORES, 2, slices * group, LANES), jnp.bfloat16),
            pltpu.VMEM(coords.shape, jnp.int32),
            pltpu.VMEM((halves * tiles * PARTS * CORES,) + block, jnp.int32),
            pltpu.VMEM((tiles * PARTS,) + block, jnp.int32),
            pltpu.VMEM((tiles, spots, slices, SUBLANES, LANES), jnp.float32),
            pltpu.VMEM(message, jnp.bfloat16),
            pltpu.VMEM(message, jnp.bfloat16),
            dma((2,)),
            dma(()),
            dma(()),
            dma(()),
            dma((halves, tiles, PARTS)),
            dma(()),
            dma(()),
            pltpu.SemaphoreType.REGULAR,
            pltpu.SemaphoreType.REGULAR,
            pltpu.SemaphoreType.REGULAR,
        ],
        compiler_params=pltpu.CompilerParams(collective_id=0, has_side_effects=True),
    )(sinogram, coords)


def solution(mesh):
    in_specs = (P("sl", "ang", None), P("ang", "sl", None))
    out_specs = P("ang", "sl", None)
    return jax.shard_map(shards, mesh=mesh, in_specs=in_specs, out_specs=out_specs, check_vma=False)
```

```python
import functools
import math

import jax
import jax.numpy as jnp
from jax import lax
from jax.experimental import pallas as pl
from jax.experimental.pallas import tpu as pltpu
from jax.sharding import PartitionSpec as P

LANES = 128
SUBLANES = 8
CORES = 2
PARTS = 2
FRACTION_BITS = 20
MESH = pl.DeviceIdType.MESH
ALONG_LANES = lax.GatherDimensionNumbers(
    offset_dims=(),
    collapsed_slice_dims=(1,),
    start_index_map=(1,),
    operand_batching_dims=(0,),
    start_indices_batching_dims=(0,),
)


def build_strip(strip, bins):
    row = lax.broadcasted_iota(jnp.int32, strip.shape, 0)
    lane = lax.broadcasted_iota(jnp.int32, strip.shape, 1)
    offset = lane - row + (bins - LANES)
    wide = offset.astype(jnp.float32)
    square = jnp.maximum(wide * wide, jnp.float32(1.0))
    odd = jnp.where((offset & 1) != 0, jnp.float32(-1.0 / math.pi**2) / square, jnp.float32(0.0))
    strip[...] = jnp.where(offset == 0, jnp.float32(0.25), odd).astype(jnp.bfloat16)


def filter_rows(sino, strip, rows_f, size):
    slices, angles, bins = sino.shape
    rows, count = slices * angles, bins // size
    blocks = [sino[:, :, i * size : (i + 1) * size].reshape(rows, size) for i in range(count)]
    totals = [None] * count
    for d in range(1 - count, count):
        inner = [i for i in range(count) if 0 <= i + d < count]
        first = bins - LANES - size * d
        right = jnp.concatenate(
            [strip[first - u : first - u + size, :] for u in range(0, size, LANES)], axis=1
        )
        left = jnp.concatenate([blocks[i] for i in inner], axis=0)
        part = jnp.dot(left, right, preferred_element_type=jnp.float32)
        for at, i in enumerate(inner):
            piece = part[at * rows : (at + 1) * rows]
            totals[i + d] = piece if totals[i + d] is None else totals[i + d] + piece
    for j, total in enumerate(totals):
        total = total.astype(jnp.bfloat16).astype(jnp.float32)
        for u in range(0, size, LANES):
            at = (j * size + u) // LANES * rows
            rows_f[at : at + rows, :] = total[:, u : u + LANES]


def build_tables(rows_f, tables_f, slices, angles):
    levels = rows_f.shape[0] // (slices * angles)
    bins = levels * LANES
    for a in range(angles):
        starts = [level * slices * angles + a for level in range(levels)]
        here = jnp.concatenate(
            [rows_f[pl.ds(at, slices, stride=angles), :] for at in starts], axis=1
        )
        following = pltpu.roll(here, bins - 1, 1)
        for v, value in enumerate((here, following)):
            for level in range(levels):
                at = pl.ds(level * angles + a, slices, stride=levels * angles)
                tables_f[v, at, :] = value[:, level * LANES : (level + 1) * LANES]


def pick(table, index):
    return lax.gather(
        table, index[..., None], ALONG_LANES, (1, 1),
        mode=lax.GatherScatterMode.PROMISE_IN_BOUNDS,
    )


def spot_weights(lines, group):
    angles = len(lines)
    row = lax.broadcasted_iota(jnp.int32, (SUBLANES, LANES), 0)
    value = jnp.broadcast_to(lines[0], (SUBLANES, LANES))
    for a in range(1, angles):
        value = jnp.where(row % angles == a, jnp.broadcast_to(lines[a], (SUBLANES, LANES)), value)
    left = value >> FRACTION_BITS
    lane, level = left & (LANES - 1), left >> 7
    right_w = (value & (2**FRACTION_BITS - 1)).astype(jnp.float32) * jnp.float32(2.0**-FRACTION_BITS)
    left_w = 1.0 - right_w
    masks = [level == (row + at) // angles for at in range(0, group, SUBLANES)]

    def stack(parts):
        return jnp.concatenate(parts, axis=0)

    return (
        stack([lane] * len(masks)).astype(jnp.int16),
        stack([jnp.where(m, left_w, 0.0) for m in masks]).astype(jnp.bfloat16),
        stack([jnp.where(m, right_w, 0.0) for m in masks]).astype(jnp.bfloat16),
    )


def fold(value):
    value = value.astype(jnp.float32)
    total = value[:SUBLANES]
    for at in range(SUBLANES, value.shape[0], SUBLANES):
        total = total + value[at : at + SUBLANES]
    return total


def spot_sums(tables, lines, slices, sums):
    group = tables.shape[1] // slices
    index, left_w, right_w = spot_weights(lines, group)
    result = []
    for s in range(slices):
        at = slice(s * group, (s + 1) * group)
        value = fold(left_w * pick(tables[0, at, :], index) + right_w * pick(tables[1, at, :], index))
        result.append(value if sums is None else sums[s] + value)
    return result


def add_rows(sums):
    row = lax.broadcasted_iota(jnp.int32, (SUBLANES, LANES), 0)

    def join(a, b, shift):
        low = (row & shift) == 0
        return jnp.where(low, a + pltpu.roll(a, SUBLANES - shift, 0), b + pltpu.roll(b, shift, 0))

    done = []
    for start in range(0, len(sums), SUBLANES):
        part = sums[start : start + SUBLANES]
        part = part + [jnp.zeros_like(part[0])] * (SUBLANES - len(part))
        for shift in (4, 2, 1):
            part = [join(part[i], part[i + shift], shift) for i in range(shift)]
        done.append(part[0])
    done = done[0] if len(done) == 1 else jnp.concatenate(done, axis=0)
    return done[: len(sums)]


def kernel(
    groups, halves, row_share, sino_hbm, coord_hbm, out, sino, strip, rows_f, tables_f, tables,
    raw, coords, stage, early, send, recv, local_sem, t_send, t_recv, c_send, c_recv, p_send, p_recv, lower_sem, next_sem, upper_sem,
):
    me, half = lax.axis_index("ang"), lax.axis_index("sl")
    core = lax.rem(me, CORES)
    mate = me + 1 - 2 * core
    slices, angles, bins = sino.shape
    tiles, per_tile, width = raw.shape[1:]
    columns = width // CORES
    share = tiles * per_tile // row_share
    across = columns // LANES
    per_step = per_tile // row_share
    part_rows = per_tile // PARTS

    def block(t, tile, part, k):
        return ((t * tiles + tile) * PARTS + part) * CORES + k

    get_sino = pltpu.make_async_copy(sino_hbm, sino, local_sem.at[0])
    get_coords = pltpu.make_async_copy(coord_hbm, raw, local_sem.at[1])
    get_sino.start()
    get_coords.start()

    quad = 2 * CORES
    place, places = me // quad, groups // quad
    barrier = pltpu.get_barrier_semaphore()

    def signal(sem, ang, sl):
        pl.semaphore_signal(sem, inc=1, device_id={"ang": ang, "sl": sl}, device_id_type=MESH)

    for t in range(1, halves):
        signal(barrier, me, lax.rem(half + t, halves))
        signal(barrier, mate, lax.rem(half + t, halves))
    for k in range(1, quad):
        signal(barrier, place * quad + lax.rem(me + k, quad), half)
    has_lower, has_upper = place > 0, place < places - 1

    @pl.when(has_lower)
    def _():
        signal(barrier, me - quad, half)

    @pl.when(has_upper)
    def _():
        for k in range(quad):
            signal(barrier, (place + 1) * quad + k, half)

    build_strip(strip, bins)
    get_sino.wait()
    filter_rows(sino, strip, rows_f, 2 * LANES)
    build_tables(rows_f, tables_f, slices, angles)
    for v in range(2):
        tables[core, v] = tables_f[v].astype(jnp.bfloat16)
    get_coords.wait()
    own_side, mate_side = (
        pl.ds(pl.multiple_of(c * columns, LANES), columns) for c in (core, 1 - core)
    )
    for tile in range(tiles):
        for part in range(PARTS):
            at = slice(part * part_rows, (part + 1) * part_rows)
            coords[block(half, tile, part, core)] = jnp.concatenate(
                [raw[a, tile, at, own_side] for a in range(angles)], axis=0
            )
            stage[tile * PARTS + part] = jnp.concatenate(
                [raw[a, tile, at, mate_side] for a in range(angles)], axis=0
            )
    beside = quad * has_lower.astype(jnp.int32) + has_upper.astype(jnp.int32)
    pl.semaphore_wait(barrier, quad - 1 + CORES * (halves - 1) + beside)

    @pl.when(jnp.logical_and(place == 1, has_upper))
    def _():
        signal(lower_sem, me + quad, half)

    @pl.when(has_lower)
    def _():
        signal(next_sem, me - quad, half)

    def remote(source, target, send_sem, recv_sem, ang, sl):
        return pltpu.make_async_remote_copy(
            src_ref=source, dst_ref=target, send_sem=send_sem, recv_sem=recv_sem,
            device_id={"ang": ang, "sl": sl}, device_id_type=MESH,
        )

    def coord_copy(tile, part, source, ang, t):
        return remote(
            source, coords.at[block(half, tile, part, core)], c_send, c_recv.at[half, tile, part],
            ang, lax.rem(half + t, halves),
        )

    def start_sides(tile, part):
        for t in range(1, halves):
            mine = coords.at[block(half, tile, part, core)]
            coord_copy(tile, part, mine, me, t).start()
            coord_copy(tile, part, stage.at[tile * PARTS + part], mate, t).start()

    chunks = [(tile, part) for tile in range(tiles) for part in range(PARTS)]
    start_sides(*chunks[0])
    for tile, part in chunks:
        coord_copy(tile, part, stage.at[tile * PARTS + part], mate, 0).start()
    mate_tables = remote(tables.at[core], tables.at[core], t_send, t_recv, mate, half)
    mate_tables.start()

    def lines(t, k, tile, r, x):
        part, at = r // part_rows, r % part_rows
        return [
            coords[
                block(t, tile, part, k), a * part_rows + at : a * part_rows + at + 1,
                x * LANES : (x + 1) * LANES,
            ]
            for a in range(angles)
        ]

    spots = [(r, x) for r in range(per_tile) for x in range(across)]

    def own_angles(tile, carry):
        for r, x in spots:
            sums = spot_sums(tables.at[core], lines(half, core, tile, r, x), slices, None)
            for s in range(slices):
                early[tile, r * across + x, s] = sums[s]

        @pl.when(tile == 0)
        def _():
            start_sides(*chunks[1])

        @pl.when(jnp.logical_and(tile == 0, jnp.logical_and(place > 1, has_upper)))
        def _():
            pl.semaphore_wait(lower_sem, 1)
            signal(lower_sem, me + quad, half)

        return carry

    lax.fori_loop(0, tiles, own_angles, 0)
    for chunk in chunks[2:3]:
        start_sides(*chunk)

    def part_copy(owner):
        return remote(send.at[owner], recv.at[me], p_send, p_recv, owner, half)

    steps = halves * tiles
    beyond = places - 1 - place
    near_step = jnp.where(place == 0, tiles - 1, 0)
    far_step = jnp.where(beyond <= 2, min(tiles, steps - 1), steps - 1)
    has_far = beyond > 1

    def step_owner(step, o):
        t, tile = step // tiles, lax.rem(step, tiles)
        return lax.rem(half + t, halves) * share + tile * per_step + o

    per_part = per_step // PARTS
    parts = [range(part * per_part, (part + 1) * per_part) for part in range(PARTS)]

    def keep(step, owners, done):
        for o in owners:
            value = jnp.concatenate(
                [
                    jnp.concatenate([done[o * row_share + i, x] for x in range(across)], axis=1)
                    for i in range(row_share)
                ],
                axis=0,
            )
            send[step_owner(step, o)] = value.astype(jnp.bfloat16)

    def deliver(step, owners, wanted):
        for o in sorted(owners, key=lambda o: o ^ 1):
            owner = step_owner(step, o)

            @pl.when(jnp.logical_and(owner != me, wanted(owner // quad)))
            def _():
                part_copy(owner).start()

    def tell_lower():
        @pl.when(has_lower)
        def _():
            signal(upper_sem, me - quad, half)

    def late(now, step, wanted):
        def one_step(earlier, carry):
            deliver(step - earlier, range(per_step), wanted)
            return carry

        lax.fori_loop(0, jnp.where(now, step + 1, 0), one_step, 0)

    def hear(step):
        now = jnp.logical_and(near_step == step, has_upper)

        @pl.when(now)
        def _():
            pl.semaphore_wait(next_sem, 1)

            @pl.when(jnp.logical_not(has_far))
            def _():
                tell_lower()

        late(now, step, lambda to: to == place + 1)
        now = jnp.logical_and(far_step == step, has_far)

        @pl.when(now)
        def _():
            pl.semaphore_wait(upper_sem, 1)
            tell_lower()

        late(now, step, lambda to: to > place + 1)

    def hear_lower(step):
        @pl.when(jnp.logical_and(step == 0, jnp.logical_and(place > 1, jnp.logical_not(has_upper))))
        def _():
            pl.semaphore_wait(lower_sem, 1)

    def run_step(step, arrived, sums_of, first):
        for part, owners in enumerate(parts):
            arrived(part)
            done = {}
            for o in owners:
                for i in range(row_share):
                    for x in range(across):
                        r = o * row_share + i
                        done[r, x] = add_rows(sums_of(r, x))
            keep(step, owners, done)
            if first and part == 0:
                hear_lower(step)
            heard = place + (near_step < step).astype(jnp.int32)
            heard = jnp.where(far_step < step, places, heard)
            deliver(step, owners, lambda to: to <= heard)

    mate_tables.wait_recv()
    for chunk in chunks[3:]:
        start_sides(*chunk)

    def coords_arrived(t, tile, part, count):
        at = pl.ds(block(t, tile, part, 0), count)
        pltpu.make_async_copy(coords.at[at], coords.at[at], c_recv.at[t, tile, part]).wait()

    def mate_angles(tile, carry):
        def arrived(part):
            coords_arrived(half, tile, part, 1)

        def sums_of(r, x):
            sums = [early[tile, r * across + x, s] for s in range(slices)]
            return spot_sums(
                tables.at[1 - core], lines(half, 1 - core, tile, r, x), slices, sums
            )

        run_step(tile, arrived, sums_of, True)
        hear(tile)
        return carry

    lax.fori_loop(0, tiles, mate_angles, 0)

    def all_angles(step, carry):
        side, tile = lax.rem(half + step // tiles, halves), lax.rem(step, tiles)

        def arrived(part):
            coords_arrived(side, tile, part, CORES)

        def sums_of(r, x):
            sums = None
            for k in range(CORES):
                sums = spot_sums(tables.at[k], lines(side, k, tile, r, x), slices, sums)
            return sums

        run_step(step, arrived, sums_of, False)
        hear(step)
        return carry

    lax.fori_loop(tiles, steps, all_angles, 0)

    others = pl.ds(0, groups - 1)
    everyone = remote(send.at[others], recv.at[others], p_send, p_recv, mate, half)
    recv[me] = send[me]
    everyone.wait_recv()
    totals = [None] * CORES
    for source in range(groups):
        value = recv[source].astype(jnp.float32)
        c = source % CORES
        totals[c] = value if totals[c] is None else totals[c] + value
    scale = jnp.float32(math.pi / (angles * groups))
    for c in range(CORES):
        total = totals[c] * scale
        for i in range(row_share):
            out[i, :, c * columns : (c + 1) * columns] = total[i * slices : (i + 1) * slices]
    mate_tables.wait_send()
    given = coords.at[pl.ds(0, len(chunks) * (1 + CORES * (halves - 1)))]
    remote(given, given, c_send, c_recv.at[0, 0, 0], mate, half).wait_send()
    everyone.wait_send()


def shards(sinogram, detector_coord):
    slices, angles, bins = sinogram.shape
    local_rows, width = detector_coord.shape[1:]
    groups, halves = lax.axis_size("ang"), lax.axis_size("sl")
    row_share = local_rows * halves // groups
    tiles, columns = local_rows // SUBLANES, width // CORES
    group = bins // LANES * angles
    coords = detector_coord.reshape(angles, tiles, SUBLANES, width)
    block = (angles * SUBLANES // PARTS, columns)
    message = (groups, row_share * slices, columns)
    spots = SUBLANES * columns // LANES
    dma = pltpu.SemaphoreType.DMA
    return pl.pallas_call(
        functools.partial(kernel, groups, halves, row_share),
        out_shape=pltpu.VMEM((row_share, slices, width), jnp.float32),
        in_specs=[pl.BlockSpec(memory_space=pl.ANY)] * 2,
        out_specs=pl.BlockSpec(memory_space=pltpu.VMEM),
        scratch_shapes=[
            pltpu.VMEM(sinogram.shape, sinogram.dtype),
            pltpu.VMEM((2 * bins - LANES, LANES), jnp.bfloat16),
            pltpu.VMEM((slices * group, LANES), jnp.float32),
            pltpu.VMEM((2, slices * group, LANES), jnp.float32),
            pltpu.VMEM((CORES, 2, slices * group, LANES), jnp.bfloat16),
            pltpu.VMEM(coords.shape, jnp.int32),
            pltpu.VMEM((halves * tiles * PARTS * CORES,) + block, jnp.int32),
            pltpu.VMEM((tiles * PARTS,) + block, jnp.int32),
            pltpu.VMEM((tiles, spots, slices, SUBLANES, LANES), jnp.float32),
            pltpu.VMEM(message, jnp.bfloat16),
            pltpu.VMEM(message, jnp.bfloat16),
            dma((2,)),
            dma(()),
            dma(()),
            dma(()),
            dma((halves, tiles, PARTS)),
            dma(()),
            dma(()),
            pltpu.SemaphoreType.REGULAR,
            pltpu.SemaphoreType.REGULAR,
            pltpu.SemaphoreType.REGULAR,
        ],
        compiler_params=pltpu.CompilerParams(collective_id=0, has_side_effects=True),
    )(sinogram, coords)


def solution(mesh):
    in_specs = (P("sl", "ang", None), P("ang", "sl", None))
    out_specs = P("ang", "sl", None)
    return jax.shard_map(shards, mesh=mesh, in_specs=in_specs, out_specs=out_specs, check_vma=False)
```
